128 devices in a mesh: arow: 8 (over z, core), acol: 16 (over x, y).
Axes of the slice: x: 4, y: 4, z: 4, core: 2. Of those that a mesh axis runs over, the one named last changes fastest.
Arguments:
- row_data: bfloat16 [262144, 128], P(('arow', 'acol')), may hold values from -96 to 96
- row_baseline: int32 [262144], P(('arow', 'acol')), may hold values from 0 to 524287, as said below
- pair_table: int32 [524288, 2], P(('arow', 'acol')), may hold values from 0 to 2047, as said below
- lengths: int32 [524288], P(('arow', 'acol')), may hold values from 1 to 8
- model_vis: bfloat16 [2048, 2048, 128], P('arow', 'acol'), may hold values from -6 to 6
- gains: float32 [2048, 128], P(('arow', 'acol')), may hold values from -6 to 6
Outputs:
- new_gains: float32 [2048, 128], P(('arow', 'acol'))
The draws below stay inside these ranges and needn't reach their ends.
Inputs may be any that keep to these rules, and one draw needn't show every extreme that they name: `pair_table`: slot j belongs to tile o = j // 4096; its first antenna lies in 256 * (o // 16) to 256 * (o // 16 + 1) - 1, its second in 128 * (o % 16) to 128 * (o % 16 + 1) - 1, and the two differ. `row_baseline`: the rows of one device name slots of one tile at most 64 times; one tile is named exactly 64 times by the rows of every device.
All inputs are finite; a program needn't handle non-finite values.
Results may differ from the reference program's by a relative error of at most 0.0003.
Values may be sent and summed in bfloat16 or wider, within the bound.
A program may use at most 64 MiB of HBM per device.

```python
import jax
import jax.numpy as jnp
from jax import lax

A = 2048
F = 64
ROWS_DEV = 2048
BPO = 4096
AR = 256
AC = 128
CAP = 64
ROWS = 262144
NBW = 524288
DEVICES = 128


def draw_pair_table(key, part):
    index = jnp.arange(NBW, dtype=jnp.int32)
    owner = index // BPO
    blocks = A // AC
    first = owner // blocks * AR + jax.random.randint(jax.random.fold_in(key, 11), (NBW,), 0, AR, dtype=jnp.int32)
    pick = jax.random.randint(jax.random.fold_in(key, 12), (NBW,), 0, AC, dtype=jnp.int32)
    second = owner % blocks * AC + pick
    second = jnp.where(second == first, owner % blocks * AC + (pick + 1) % AC, second)
    return jnp.stack([first, second], axis=1)


def draw_row_baseline(key, part):
    spots = jnp.arange(ROWS_DEV, dtype=jnp.int32)
    flips = jax.random.randint(jax.random.fold_in(key, 21), (DEVICES, ROWS_DEV), 0, 2, dtype=jnp.int32)
    rest = spots[None, :] - CAP
    ranking = jnp.where(spots[None, :] < CAP, 0, 1 + (rest % (DEVICES - 1) + flips) % (DEVICES - 1))
    streams = jax.random.split(jax.random.fold_in(key, 22), DEVICES)
    mixed = jax.vmap(lambda stream, row: row[jax.random.permutation(stream, ROWS_DEV)])(streams, ranking)
    chosen = jax.random.permutation(jax.random.fold_in(key, 23), DEVICES).astype(jnp.int32)
    owner = chosen[mixed]
    pick = jax.random.randint(jax.random.fold_in(key, 24), (DEVICES, ROWS_DEV), 0, BPO, dtype=jnp.int32)
    return (owner * BPO + pick).reshape(ROWS).astype(jnp.int32)


def set_ends(result, stream_key, low, high):
    longest = result.shape.index(max(result.shape))
    spots = []
    for shift in (0, 1):
        where = [jax.random.randint(jax.random.fold_in(stream_key, axis), (), 0, length) for axis, length in enumerate(result.shape)]
        where[longest] = (where[longest] + shift) % result.shape[longest]
        spots.append(tuple(where))
    return result.at[spots[0]].set(low).at[spots[1]].set(high)


def levels(stream_key, shape, cuts, smallest, high):
    gain = 1.0
    for axis_at, shards_of in cuts:
        heights = jax.random.uniform(jax.random.fold_in(jax.random.fold_in(stream_key, 6), axis_at), (shards_of,), jnp.float32, smallest / len(cuts), high / len(cuts))
        gain = gain * jnp.repeat(jnp.exp(heights), shape[axis_at] // shards_of).reshape((-1,) + (1,) * (len(shape) - 1 - axis_at))
    return gain


def noise(stream_key, extent, spread, bound, pieces=(), held_as=jnp.bfloat16):
    entries = jax.random.normal(stream_key, extent, jnp.float32) * spread
    if len(pieces) > 0:
        entries = levels(stream_key, extent, pieces, -0.22, 0.18) * entries
    return jnp.clip(entries, min=-bound, max=bound).astype(held_as)


def setup_inputs(seed: int = 0) -> dict:
    streams_of = jax.random.split(jax.random.key(seed), 7)
    return {
        "row_data": noise(streams_of[0], (ROWS, 2 * F), 16.0, 96.0, ((0, 128),)),
        "row_baseline": draw_row_baseline(jax.random.fold_in(streams_of[6], 71), 0),
        "pair_table": draw_pair_table(jax.random.fold_in(streams_of[6], 71), 0),
        "lengths": set_ends(jax.random.randint(streams_of[3], (NBW,), 1, 9), jax.random.fold_in(streams_of[3], 1), 1, 8).astype(jnp.int32),
        "model_vis": noise(streams_of[4], (A, A, 2 * F), 1.0, 6.0, ((0, 8), (1, 16))),
        "gains": noise(streams_of[5], (A, 2 * F), 1.0, 6.0, ((0, 128),), jnp.float32),
    }


def reference(row_data, row_baseline, pair_table, lengths, model_vis, gains):
    pairs = pair_table[row_baseline]
    first = pairs[:, 0]
    second = pairs[:, 1]
    weight = lengths[row_baseline].astype(jnp.float32)
    terms = weight[:, None] * row_data.astype(jnp.float32)
    nant = gains.shape[0]
    half = gains.shape[1] // 2
    band = nant // 8
    g_re = gains[None, :, :half]
    g_im = gains[None, :, half:]

    def block(index):
        start = index * band
        local = first - start
        inside = (local >= 0) & (local < band)
        spot = jnp.where(inside, local * nant + second, band * nant)
        sums = jnp.zeros((band * nant + 1, 2 * half), jnp.float32).at[spot].add(terms)
        sums = sums[:-1].reshape(band, nant, 2 * half)
        totals = jnp.zeros((band * nant + 1,), jnp.float32).at[spot].add(weight)
        totals = totals[:-1].reshape(band, nant)
        model = lax.dynamic_slice_in_dim(model_vis, start, band, 0)
        m_re = model[..., :half].astype(jnp.float32)
        m_im = model[..., half:].astype(jnp.float32)
        c_re = m_re * g_re + m_im * g_im
        c_im = m_re * g_im - m_im * g_re
        s_re = sums[..., :half]
        s_im = sums[..., half:]
        num = jnp.concatenate([jnp.sum(c_re * s_re - c_im * s_im, axis=1), jnp.sum(c_re * s_im + c_im * s_re, axis=1)], axis=1)
        den = jnp.sum(totals[:, :, None] * (c_re * c_re + c_im * c_im), axis=1)
        return num, den

    nums, dens = lax.map(block, jnp.arange(8, dtype=jnp.int32))
    num = nums.reshape(nant, 2 * half)
    den = dens.reshape(nant, half)
    return jnp.concatenate([num[:, :half] / (den + 1.0), num[:, half:] / (den + 1.0)], axis=1)
```

```python
import functools

import jax
import jax.numpy as jnp
from jax import lax
from jax.experimental import pallas as pl
from jax.experimental.pallas import tpu as pltpu
from jax.sharding import PartitionSpec as P

MESH = pl.DeviceIdType.MESH
RIDGE = 1.0
F32 = jnp.float32
BF16 = jnp.bfloat16
I32 = jnp.int32

ROWS = 2048
CAP = 64
SLOTS = 4096
AR = 256
AC = 128
HALF = 64
DEVICES = 128
GROUPS = 32
CHUNKS = 8
DY = (2, 1, 3, 0)
SELF_GROUP = 20
SELF_SLOT = 83


def far_first(a):
    return lax.rem(2 + 3 * a, 4)


def place():
    row = lax.axis_index("arow")
    col = lax.axis_index("acol")
    return row, col


def destination(g):
    row, col = place()
    z = lax.rem(row // 2 + far_first(g // 8), 4)
    core = lax.rem(row + lax.rem(g, 2), 2)
    x = lax.rem(col // 4 + far_first(lax.rem(g // 2, 4)), 4)
    return 2 * z + core, x


def iota(shape, dim):
    return lax.broadcasted_iota(I32, shape, dim)


def one_hot(match):
    return jnp.where(match, F32(1), F32(0)).astype(BF16)


def split_two(value):
    high = value.astype(BF16)
    return high, (value - high.astype(F32)).astype(BF16)


def kernel(
    x_hbm, rb_hbm, pair_hbm, len_hbm, m_hbm, g_hbm, out_ref,
    x_v, rb_v, pair_v, len_v, mb_v, mf_v, idx_v, idx_s, msel, xt, tgt,
    send, sendc, recv, recvc, gcol, cre, cim, den, codes, lhs, cb, acc,
    part, got,
    in_sem, m_sem, idx_sem, g_sem, gs_sem, d_ssem, d_rsem, c_ssem, c_rsem, r_ssem, r_rsem,
):
    row, col = place()
    me = row * 16 + col
    y = lax.rem(col, 4)

    barrier = pltpu.get_barrier_semaphore()

    @pl.loop(0, GROUPS)
    def _(g):
        r2, x2 = destination(g)
        for dy in DY:
            y2 = lax.rem(y + dy, 4)
            if dy:
                pl.semaphore_signal(barrier, 1, device_id=(r2, 4 * x2 + y2), device_id_type=MESH)
            else:
                @pl.when(g != SELF_GROUP)
                def _():
                    pl.semaphore_signal(barrier, 1, device_id=(r2, 4 * x2 + y2), device_id_type=MESH)

    loads = [
        pltpu.make_async_copy(rb_hbm, rb_v, in_sem.at[0]),
        pltpu.make_async_copy(pair_hbm, pair_v, in_sem.at[1]),
        pltpu.make_async_copy(x_hbm, x_v, in_sem.at[2]),
        pltpu.make_async_copy(len_hbm, len_v, in_sem.at[3]),
    ]
    for load in loads:
        load.start()
    m_loads = [
        pltpu.make_async_copy(m_hbm.at[pl.ds(j * 4096, 4096)], mb_v.at[pl.ds(j * 4096, 4096)], m_sem.at[j])
        for j in range(8)
    ]
    for load in m_loads:
        load.start()

    loads[0].wait()
    slots = rb_v[...]
    owner = slots // SLOTS
    local = slots - owner * SLOTS + 1
    owner_t = owner.astype(F32).T
    lower = one_hot(iota((256, 256), 0) > iota((256, 256), 1))
    ones = jnp.ones((128, 128), BF16)
    lane = iota((128, 128), 1).astype(F32)
    before = jnp.zeros((1, 128), F32)
    for b in range(8):
        own = jnp.concatenate(
            [jnp.broadcast_to(owner_t[:, 2 * b + h : 2 * b + h + 1], (128, 128)) for h in range(2)], axis=0
        )
        hit = jnp.where(own == jnp.concatenate([lane, lane], axis=0), F32(1), F32(0))
        within = jnp.dot(lower, hit.astype(BF16), preferred_element_type=F32)
        rank = jnp.dot((hit * (within + before)).astype(BF16), ones, preferred_element_type=F32)
        tgt[b * 256 : b * 256 + 256, :] = (own * CAP + rank).astype(I32)
        before = before + within[255:256, :] + hit[255:256, :]

    loads[1].wait()
    for k in range(32):
        p = pair_v[0:1, k * 128 : k * 128 + 128] - row * AR
        q = pair_v[1:2, k * 128 : k * 128 + 128] - col * AC
        idx_v[k : k + 1, :] = jnp.clip(p * AC + q, 0, AR * AC - 1)
    idx_copy = pltpu.make_async_copy(idx_v, idx_s, idx_sem)
    idx_copy.start()

    loads[2].wait()
    sub = iota((16, 128), 0)
    for b in range(16):
        xt[0:128, b * 128 : b * 128 + 128] = x_v[b * 128 : b * 128 + 128, :].T
        code = local[b : b + 1, :]
        high = code // 64
        digits = jnp.where(sub == 0, high, jnp.where(sub == 1, code - high * 64, 0))
        xt[128:144, b * 128 : b * 128 + 128] = digits.astype(F32).astype(BF16)

    pl.semaphore_wait(barrier, DEVICES - 1)

    g_col = me // 8
    g_at = pl.ds(pl.multiple_of(lax.rem(me, 8) * 16, 16), 16)
    for r2 in range(8):
        @pl.when(jnp.logical_or(row != r2, col != g_col))
        def _():
            pltpu.make_async_remote_copy(
                src_ref=g_hbm, dst_ref=gcol.at[g_at], send_sem=gs_sem, recv_sem=g_sem,
                device_id=(r2, g_col), device_id_type=MESH,
            ).start()

    @pl.when(col == g_col)
    def _():
        pltpu.make_async_copy(g_hbm, gcol.at[g_at], g_sem).start()

    low_lanes = iota((HALF, 128), 1) < HALF

    def pack(g):
        r2, x2 = destination(g)
        group = r2 * 4 + x2
        total = None
        for kb in range(8):
            rows = tgt[kb * 256 : kb * 256 + 256, :]
            hot = jnp.concatenate(
                [one_hot(rows == iota((256, 128), 1) + (group * 256 + h * 128)) for h in range(2)], axis=1
            )
            term = jnp.dot(xt[:, kb * 256 : kb * 256 + 256], hot, preferred_element_type=F32)
            total = term if total is None else total + term
        for h in range(2):
            re = total[0:64, h * 128 : h * 128 + 128]
            im = total[64:128, h * 128 : h * 128 + 128]
            send[group * 4 + 2 * h] = jnp.where(low_lanes, re, pltpu.roll(im, 64, 1)).astype(BF16)
            send[group * 4 + 2 * h + 1] = jnp.where(low_lanes, pltpu.roll(re, 64, 1), im).astype(BF16)
            code = total[128:129, h * 128 : h * 128 + 128] * 64.0 + total[129:130, h * 128 : h * 128 + 128]
            sendc[group * 2 + h] = code.astype(I32) - 1

    def ship(g):
        r2, x2 = destination(g)
        group = r2 * 4 + x2
        chunk = g // 4
        for k, dy in enumerate(DY):
            y2 = lax.rem(y + dy, 4)

            def go():
                pltpu.make_async_remote_copy(
                    src_ref=sendc.at[group * 2 + y2 // 2], dst_ref=recvc.at[g * 4 + k],
                    send_sem=c_ssem, recv_sem=c_rsem.at[chunk],
                    device_id=(r2, 4 * x2 + y2), device_id_type=MESH,
                ).start()
                pltpu.make_async_remote_copy(
                    src_ref=send.at[group * 4 + y2], dst_ref=recv.at[g * 4 + k],
                    send_sem=d_ssem, recv_sem=d_rsem.at[chunk],
                    device_id=(r2, 4 * x2 + y2), device_id_type=MESH,
                ).start()

            if dy:
                go()
            else:
                pl.when(g != SELF_GROUP)(go)

    pack(jnp.int32(0))

    @pl.loop(1, GROUPS)
    def _(g):
        pack(g)
        ship(g - 1)

    ship(jnp.int32(GROUPS - 1))
    recv[SELF_SLOT] = send[me]
    recvc[SELF_SLOT] = sendc[me // 2]

    for j in range(8):
        m_loads[j].wait()

        @pl.loop(0, 16)
        def _(b):
            at = pl.ds(pl.multiple_of(j * 4096 + b * 256, 256), 256)
            mf_v[at, :] = mb_v[at, :].astype(F32)

    idx_copy.wait()

    @pl.loop(0, 64)
    def _(b):
        for u in range(64):
            i = idx_s[b // 2, lax.rem(b, 2) * 64 + u]
            msel[pl.ds(b * 64 + u, 1), :] = mf_v[pl.ds(i, 1), :]

    loads[3].wait()
    pltpu.make_async_copy(gcol, gcol, g_sem).wait()
    gains_two = jnp.concatenate(split_two(gcol[...].T), axis=0)
    for k in range(32):
        at = slice(k * 128, k * 128 + 128)
        q = pair_v[1:2, at] - col * AC
        picked = jnp.dot(gains_two, one_hot(iota((128, 128), 0) == q), preferred_element_type=F32)
        g_re = picked[0:64] + picked[128:192]
        g_im = picked[64:128] + picked[192:256]
        model = msel[at, :].T
        m_re = model[0:64]
        m_im = model[64:128]
        c_re = m_re * g_re + m_im * g_im
        c_im = m_re * g_im - m_im * g_re
        w = len_v[k : k + 1, :].astype(F32)
        cre[:, at] = w * c_re
        cim[:, at] = w * c_im
        den[:, at] = w * (c_re * c_re + c_im * c_im)

    acc[...] = jnp.zeros_like(acc)
    lhs[128:144, :] = jnp.ones((16, 1024), BF16)
    odd = lax.rem(col, 2) == 1
    first_lanes = iota((1, 128), 1) < HALF

    def add_chunk(j, senders):
        pltpu.make_async_copy(recv.at[pl.ds(0, senders)], recv.at[pl.ds(0, senders)], d_rsem.at[j]).wait()
        pltpu.make_async_copy(recvc.at[pl.ds(0, senders)], recvc.at[pl.ds(0, senders)], c_rsem.at[j]).wait()
        for s in range(8):
            a = recv[j * 16 + 2 * s].astype(F32)
            b = recv[j * 16 + 2 * s + 1].astype(F32)
            at = slice(s * 128, s * 128 + 128)
            lhs[0:64, at] = jnp.where(low_lanes, a, pltpu.roll(b, 64, 1)).astype(BF16)
            lhs[64:128, at] = jnp.where(low_lanes, pltpu.roll(a, 64, 1), b).astype(BF16)
            ca = recvc[j * 16 + 2 * s]
            cbb = recvc[j * 16 + 2 * s + 1]
            even_codes = jnp.where(first_lanes, ca, pltpu.roll(cbb, 64, 1))
            odd_codes = jnp.where(first_lanes, pltpu.roll(ca, 64, 1), cbb)
            codes[s : s + 1, :] = jnp.where(odd, odd_codes, even_codes)
        codes_t = codes[...].astype(F32).T
        for s in range(8):
            cb[s * 128 : s * 128 + 128, :] = jnp.broadcast_to(codes_t[:, s : s + 1], (128, 128)).astype(I32)
        for nb in range(16):
            total = None
            for kb in range(4):
                rows = cb[kb * 256 : kb * 256 + 256, :]
                hot = jnp.concatenate(
                    [one_hot(rows == iota((256, 128), 1) + (nb * 256 + h * 128)) for h in range(2)], axis=1
                )
                term = jnp.dot(lhs[:, kb * 256 : kb * 256 + 256], hot, preferred_element_type=F32)
                total = term if total is None else total + term
            acc[:, nb * 256 : nb * 256 + 256] += total

    @pl.loop(0, CHUNKS)
    def _(j):
        @pl.when(j == SELF_SLOT // 16)
        def _():
            add_chunk(j, 15)

        @pl.when(j != SELF_SLOT // 16)
        def _():
            add_chunk(j, 16)

    total = None
    for nb in range(16):
        at = slice(nb * 256, nb * 256 + 256)
        d_re = acc[0:64, at]
        d_im = acc[64:128, at]
        v = jnp.concatenate(
            [cre[:, at] * d_re - cim[:, at] * d_im, cre[:, at] * d_im + cim[:, at] * d_re, den[:, at] * acc[128:129, at]],
            axis=0,
        )
        both = jnp.concatenate(split_two(v), axis=0)
        p = pair_v[0:1, at] - row * AR
        hot = one_hot(iota((AR, 256), 0) == p)
        term = lax.dot_general(hot, both, (((1,), (1,)), ((), ())), preferred_element_type=F32)
        total = term if total is None else total + term
    numer = total[:, 0:128] + total[:, 192:320]
    denom = total[:, 128:192] + total[:, 320:384]
    wide = jnp.concatenate([denom, denom], axis=1)
    eight = iota((8, 128), 1) < HALF
    for b in range(16):
        part[b, 0:16, :] = numer[b * 16 : b * 16 + 16]
        part[b, 16:24, :] = jnp.where(eight, wide[b * 16 : b * 16 + 8], wide[b * 16 + 8 : b * 16 + 16])

    for k in range(1, 16):
        x2 = lax.rem(col // 4 + k // 4, 4)
        y2 = lax.rem(y + k, 4)
        pltpu.make_async_remote_copy(
            src_ref=part.at[4 * x2 + y2], dst_ref=got.at[k], send_sem=r_ssem, recv_sem=r_rsem,
            device_id=(row, 4 * x2 + y2), device_id_type=MESH,
        ).start()
    result = part[col]
    pltpu.make_async_copy(got.at[pl.ds(1, 15)], got.at[pl.ds(1, 15)], r_rsem).wait()
    for k in range(1, 16):
        result = result + got[k]
    d8 = result[16:24] + RIDGE
    d8r = pltpu.roll(d8, 64, 1)
    out_ref[0:8, :] = result[0:8] / jnp.where(eight, d8, d8r)
    out_ref[8:16, :] = result[8:16] / jnp.where(eight, d8r, d8)

    pltpu.make_async_copy(send.at[pl.ds(0, 127)], send.at[pl.ds(0, 127)], d_ssem).wait()
    pltpu.make_async_copy(recvc.at[pl.ds(0, 127)], recvc.at[pl.ds(0, 127)], c_ssem).wait()
    pltpu.make_async_copy(part.at[pl.ds(0, 15)], part.at[pl.ds(0, 15)], r_ssem).wait()

    @pl.when(col == g_col)
    def _():
        pltpu.make_async_copy(gcol.at[pl.ds(0, 112)], gcol.at[pl.ds(0, 112)], gs_sem).wait()

    @pl.when(col != g_col)
    def _():
        pltpu.make_async_copy(gcol, gcol, gs_sem).wait()


def local_step(row_data, row_baseline, pair_table, lengths, model_vis, gains):
    any_space = pl.BlockSpec(memory_space=pl.ANY)
    vm = pltpu.VMEM
    dma = pltpu.SemaphoreType.DMA
    return pl.pallas_call(
        kernel,
        out_shape=jax.ShapeDtypeStruct((16, 128), F32),
        in_specs=[any_space] * 6,
        out_specs=pl.BlockSpec(memory_space=pltpu.VMEM),
        scratch_shapes=[
            vm((ROWS, 128), BF16), vm((16, 128), I32), vm((2, SLOTS), I32), vm((32, 128), I32),
            vm((AR * AC, 128), BF16), vm((AR * AC, 128), F32),
            vm((32, 128), I32), pltpu.SMEM((32, 128), I32), vm((SLOTS, 128), F32),
            vm((144, ROWS), BF16), vm((ROWS, 128), I32),
            vm((DEVICES, HALF, 128), BF16), vm((DEVICES // 2, 1, 128), I32),
            vm((DEVICES, HALF, 128), BF16), vm((DEVICES, 1, 128), I32),
            vm((AC, 128), F32),
            vm((HALF, SLOTS), F32), vm((HALF, SLOTS), F32), vm((HALF, SLOTS), F32),
            vm((8, 128), I32), vm((144, 1024), BF16), vm((1024, 128), I32), vm((144, SLOTS), F32),
            vm((16, 24, 128), F32), vm((16, 24, 128), F32),
            dma((4,)), dma((8,)), dma, dma, dma, dma, dma((CHUNKS,)), dma, dma((CHUNKS,)), dma, dma,
        ],
        compiler_params=pltpu.CompilerParams(
            collective_id=0, has_side_effects=True, vmem_limit_bytes=60 * 2**20
        ),
    )(
        row_data,
        row_baseline.reshape(16, 128),
        pair_table.T,
        lengths.reshape(32, 128),
        model_vis.reshape(AR * AC, 128),
        gains,
    )


def solution(mesh):
    rows = P(("arow", "acol"))
    placed = (
        P(("arow", "acol"), None),
        rows,
        P(("arow", "acol"), None),
        rows,
        P("arow", "acol", None),
        P(("arow", "acol"), None),
    )
    return jax.shard_map(
        local_step, mesh=mesh, in_specs=placed, out_specs=P(("arow", "acol"), None), check_vma=False
    )
```

```python
import itertools

import jax
import jax.numpy as jnp
from jax import lax
from jax.experimental import pallas as pl
from jax.experimental.pallas import tpu as pltpu
from jax.sharding import PartitionSpec as P

MESH = pl.DeviceIdType.MESH
RIDGE = 1.0
F32 = jnp.float32
BF16 = jnp.bfloat16
I32 = jnp.int32

ROWS = 2048
CAP = 64
SLOTS = 4096
AR = 256
AC = 128
HALF = 64
DEVICES = 128
CHUNKS = 8
SELF = 127


def place():
    row = lax.axis_index("arow")
    col = lax.axis_index("acol")
    return row, col


def near_first():
    hops = (0, 1, 2, 1)

    def loads(offset):
        load = [0] * 6
        for axis, d in enumerate((offset[0], offset[2], offset[3])):
            if d != 3:
                load[2 * axis] += min(d, 1)
            if d > 1:
                load[2 * axis + 1] += 1
        return load

    left = [o for o in itertools.product(range(4), range(2), range(4), range(4)) if any(o)]
    order, total = [], [0] * 6
    while left:
        near = min(hops[o[0]] + hops[o[2]] + hops[o[3]] for o in left)

        def cost(o):
            after = [t + n for t, n in zip(total, loads(o))]
            return max(after), sum(a * a for a in after), o

        best = min((o for o in left if hops[o[0]] + hops[o[2]] + hops[o[3]] == near), key=cost)
        left.remove(best)
        order.append(best)
        total = [t + n for t, n in zip(total, loads(best))]
    return order + [(0, 0, 0, 0)]


ORDER = near_first()


def offset_of(owner):
    row, col = place()
    z = (owner // 32 - row // 2) & 3
    core = (owner // 16 - row) & 1
    x = (owner // 4 - col // 4) & 3
    return 32 * z + 16 * core + 4 * x + ((owner - col) & 3)


def each_tile(places, act):
    row, col = place()
    rows = [[2 * lax.rem(row // 2 + z, 4) + lax.rem(row + core, 2) for core in range(2)] for z in range(4)]
    xs = [4 * lax.rem(col // 4 + d, 4) for d in range(4)]
    ys = [lax.rem(col + d, 4) for d in range(4)]
    for pos in places:
        if pos != SELF:
            z, core, x, y = ORDER[pos]
            act(pos, (rows[z][core], xs[x] + ys[y]))


def iota(shape, dim):
    return lax.broadcasted_iota(I32, shape, dim)


def one_hot(match):
    return jnp.where(match, F32(1), F32(0)).astype(BF16)


def split_two(value):
    high = value.astype(BF16)
    return high, (value - high.astype(F32)).astype(BF16)


def kernel(
    x_hbm, rb_hbm, pair_hbm, len_hbm, m_hbm, g_hbm, order_hbm, out_ref,
    order_v, x_v, rb_v, pair_v, len_v, mb_v, mf_v, idx_v, idx_s, msel, xt, tgt,
    send, sendc, recv, recvc, gcol, cre, cim, den, codes, lhs, cb, acc,
    part, got, raw, gains_two,
    in_sem, m_sem, idx_sem, g_sem, gs_sem, g2_sem, gs2_sem, d_ssem, d_rsem, c_ssem, c_rsem, r_ssem, r_rsem,
):
    row, col = place()
    me = row * 16 + col

    loads = [
        pltpu.make_async_copy(rb_hbm, rb_v, in_sem.at[0]),
        pltpu.make_async_copy(pair_hbm, pair_v, in_sem.at[1]),
        pltpu.make_async_copy(x_hbm, x_v, in_sem.at[2]),
        pltpu.make_async_copy(len_hbm, len_v, in_sem.at[3]),
        pltpu.make_async_copy(order_hbm, order_v, in_sem.at[4]),
    ]
    for load in loads:
        load.start()
    m_loads = [
        pltpu.make_async_copy(m_hbm.at[pl.ds(j * 4096, 4096)], mb_v.at[pl.ds(j * 4096, 4096)], m_sem.at[j])
        for j in range(8)
    ]
    for load in m_loads:
        load.start()

    barrier = pltpu.get_barrier_semaphore()

    each_tile(
        range(DEVICES - 1, -1, -1),
        lambda pos, peer: pl.semaphore_signal(barrier, 1, device_id=peer, device_id_type=MESH),
    )

    loads[0].wait()
    slots = rb_v[...]
    owner = slots // SLOTS
    local = slots - owner * SLOTS + 1
    owner_t = offset_of(owner).astype(F32).T
    loads[4].wait()
    places = order_v[...]
    lower = one_hot(iota((256, 256), 0) > iota((256, 256), 1))
    spread = jnp.where(iota((256, 128), 0) < 128, F32(1), F32(CAP)).astype(BF16)
    lane = iota((256, 128), 1).astype(F32)
    before = jnp.zeros((1, 128), F32)
    for b in range(8):
        own = jnp.concatenate(
            [jnp.broadcast_to(owner_t[:, 2 * b + h : 2 * b + h + 1], (128, 128)) for h in range(2)], axis=0
        )
        hit = jnp.where(own == places, F32(1), F32(0))
        within = jnp.dot(lower, hit.astype(BF16), preferred_element_type=F32)
        two = jnp.concatenate([(hit * (within + before)).astype(BF16), (hit * lane).astype(BF16)], axis=1)
        tgt[b * 256 : b * 256 + 256, :] = jnp.dot(two, spread, preferred_element_type=F32).astype(I32)
        before = before + within[255:256, :] + hit[255:256, :]

    loads[1].wait()
    for k in range(32):
        p = pair_v[0:1, k * 128 : k * 128 + 128] - row * AR
        q = pair_v[1:2, k * 128 : k * 128 + 128] - col * AC
        idx_v[k : k + 1, :] = jnp.clip(p * AC + q, 0, AR * AC - 1)
    idx_copy = pltpu.make_async_copy(idx_v, idx_s, idx_sem)
    idx_copy.start()

    loads[2].wait()
    sub = iota((16, 128), 0)
    for b in range(16):
        xt[0:128, b * 128 : b * 128 + 128] = x_v[b * 128 : b * 128 + 128, :].T
        code = local[b : b + 1, :]
        high = code // 64
        digits = jnp.where(sub == 0, high, jnp.where(sub == 1, code - high * 64, 0))
        xt[128:144, b * 128 : b * 128 + 128] = digits.astype(F32).astype(BF16)

    acc[...] = jnp.zeros_like(acc)
    lhs[128:144, :] = jnp.ones((16, 1024), BF16)
    low_lanes = iota((HALF, 128), 1) < HALF

    def multiply(c, k):
        total = None
        for kb in range(8):
            rows = tgt[kb * 256 : kb * 256 + 256, :]
            hot = jnp.concatenate(
                [one_hot(rows == iota((256, 128), 1) + (c * 1024 + k * 256 + h * 128)) for h in range(2)], axis=1
            )
            term = jnp.dot(xt[:, kb * 256 : kb * 256 + 256], hot, preferred_element_type=F32)
            total = term if total is None else total + term
        raw[k] = total

    def arrange(c, k):
        for h in range(2):
            at = slice(h * 128, h * 128 + 128)
            re = raw[k, 0:64, at]
            im = pltpu.roll(raw[k, 64:128, at], 64, 1)
            send[c * 16 + k * 4 + 2 * h] = jnp.where(low_lanes, re, im).astype(BF16)
            send[c * 16 + k * 4 + 2 * h + 1] = jnp.where(low_lanes, im, re).astype(BF16)
            code = raw[k, 128:129, at] * 64.0 + raw[k, 129:130, at]
            sendc[c * 8 + k * 2 + h] = code.astype(I32) - 1

    def pack(c, beside):
        for k in range(4):
            multiply(c, k)
            beside(k)
            if k:
                arrange(c, k - 1)
        arrange(c, 3)

    def ship(c):
        def go(pos, peer):
            pltpu.make_async_remote_copy(
                src_ref=sendc.at[pos // 2], dst_ref=recvc.at[pos],
                send_sem=c_ssem, recv_sem=c_rsem.at[c], device_id=peer, device_id_type=MESH,
            ).start()
            pltpu.make_async_remote_copy(
                src_ref=send.at[pos], dst_ref=recv.at[pos],
                send_sem=d_ssem, recv_sem=d_rsem.at[c], device_id=peer, device_id_type=MESH,
            ).start()

        each_tile(range(c * 16, c * 16 + 16), go)

    def widen(at, count):
        at = pl.ds(pl.multiple_of(at, 1024), count)
        mf_v[at, :] = mb_v[at, :].astype(F32)

    def wait_model(j):
        at = pl.ds(pl.multiple_of(j * 4096, 4096), 4096)
        pltpu.make_async_copy(m_hbm.at[at], mb_v.at[at], m_sem.at[j]).wait()

    pack(0, lambda k: None)
    pl.semaphore_wait(barrier, DEVICES - 1)

    g_row = lax.rem(me, 8)
    g_col = me // 8
    g_at = pl.ds(pl.multiple_of(g_row * 16, 16), 16)
    g_mine = jnp.logical_and(row == g_row, col == g_col)

    @pl.when(g_mine)
    def _():
        pltpu.make_async_copy(g_hbm, gcol.at[g_at], g_sem).start()

    @pl.when(jnp.logical_not(g_mine))
    def _():
        pltpu.make_async_remote_copy(
            src_ref=g_hbm, dst_ref=gcol.at[g_at], send_sem=gs_sem, recv_sem=g_sem,
            device_id=(g_row, g_col), device_id_type=MESH,
        ).start()

    ship(0)

    @pl.loop(1, CHUNKS)
    def _(c):
        wait_model(c)
        pack(c, lambda k: widen(c * 4096 + k * 1024, 1024))

        @pl.when(c == 4)
        def _():
            pltpu.make_async_copy(gcol.at[pl.ds(0, 16)], gcol.at[pl.ds(0, 16)], g_sem).wait()
            my_gains = gcol.at[pl.ds(pl.multiple_of(row * 16, 16), 16)]
            for k in range(1, 8):
                pltpu.make_async_remote_copy(
                    src_ref=my_gains, dst_ref=my_gains, send_sem=gs2_sem, recv_sem=g2_sem,
                    device_id=(lax.rem(row + k, 8), col), device_id_type=MESH,
                ).start()

        for k in range(1, CHUNKS):
            @pl.when(c == k)
            def _():
                ship(k)

    wait_model(0)
    widen(0, 4096)
    idx_copy.wait()
    loads[3].wait()

    first_lanes = iota((1, 128), 1) < HALF

    def gather(block, u0, count):
        for u in range(u0, u0 + count):
            i = idx_s[block, u]
            msel[pl.ds(block * 128 + u, 1), :] = mf_v[pl.ds(i, 1), :]

    def slot_terms(block, gains_two):
        at = pl.ds(pl.multiple_of(block * 128, 128), 128)
        q = pair_v[1:2, at] - col * AC
        picked = jnp.dot(gains_two, one_hot(iota((128, 128), 0) == q), preferred_element_type=F32)
        g_re = picked[0:64] + picked[128:192]
        g_im = picked[64:128] + picked[192:256]
        model = msel[at, :].T
        m_re = model[0:64]
        m_im = model[64:128]
        c_re = m_re * g_re + m_im * g_im
        c_im = m_re * g_im - m_im * g_re
        w = len_v[pl.ds(block, 1), :].astype(F32)
        cre[:, at] = w * c_re
        cim[:, at] = w * c_im
        den[:, at] = w * (c_re * c_re + c_im * c_im)

    def arrived(j, senders):
        pltpu.make_async_copy(recv.at[pl.ds(0, senders)], recv.at[pl.ds(0, senders)], d_rsem.at[j]).wait()
        pltpu.make_async_copy(recvc.at[pl.ds(0, senders)], recvc.at[pl.ds(0, senders)], c_rsem.at[j]).wait()

    def add_chunk(j, beside):
        for s in range(8):
            a = recv[j * 16 + 2 * s].astype(F32)
            b = recv[j * 16 + 2 * s + 1].astype(F32)
            at = slice(s * 128, s * 128 + 128)
            lhs[0:64, at] = jnp.where(low_lanes, a, b).astype(BF16)
            lhs[64:128, at] = pltpu.roll(jnp.where(low_lanes, b, a), 64, 1).astype(BF16)
            codes[s : s + 1, :] = jnp.where(first_lanes, recvc[j * 16 + 2 * s], recvc[j * 16 + 2 * s + 1])
        codes_t = codes[...].astype(F32).T
        for s in range(8):
            cb[s * 128 : s * 128 + 128, :] = jnp.broadcast_to(codes_t[:, s : s + 1], (128, 128)).astype(I32)
        for nb in range(16):
            total = None
            for kb in range(4):
                rows = cb[kb * 256 : kb * 256 + 256, :]
                hot = jnp.concatenate(
                    [one_hot(rows == iota((256, 128), 1) + (nb * 256 + h * 128)) for h in range(2)], axis=1
                )
                term = jnp.dot(lhs[:, kb * 256 : kb * 256 + 256], hot, preferred_element_type=F32)
                total = term if total is None else total + term
            acc[:, nb * 256 : nb * 256 + 256] += total
            beside(nb)

    @pl.loop(0, 4)
    def _(j):
        arrived(j, 16)
        add_chunk(j, lambda nb: gather(j * 8 + nb // 2, nb % 2 * 64, 64))

    recv[SELF] = send[SELF]
    recvc[SELF] = sendc[SELF // 2]
    pltpu.make_async_copy(gcol.at[pl.ds(0, 112)], gcol.at[pl.ds(0, 112)], g2_sem).wait()
    gains_two[...] = jnp.concatenate(split_two(gcol[...].T), axis=0)

    @pl.loop(4, 7)
    def _(j):
        arrived(j, 16)

        def beside(nb):
            if nb < 11:
                slot_terms(jnp.minimum((j - 4) * 11 + nb, 31), gains_two[...])

        add_chunk(j, beside)

    arrived(7, 15)
    add_chunk(7, lambda nb: None)

    total = None
    for nb in range(16):
        at = slice(nb * 256, nb * 256 + 256)
        d_re = acc[0:64, at]
        d_im = acc[64:128, at]
        v = jnp.concatenate(
            [cre[:, at] * d_re - cim[:, at] * d_im, cre[:, at] * d_im + cim[:, at] * d_re, den[:, at] * acc[128:129, at]],
            axis=0,
        )
        both = jnp.concatenate(split_two(v), axis=0)
        p = pair_v[0:1, at] - row * AR
        hot = one_hot(iota((AR, 256), 0) == p)
        term = lax.dot_general(hot, both, (((1,), (1,)), ((), ())), preferred_element_type=F32)
        total = term if total is None else total + term
    numer = total[:, 0:128] + total[:, 192:320]
    denom = total[:, 128:192] + total[:, 320:384]
    wide = jnp.concatenate([denom, denom], axis=1)
    eight = iota((8, 128), 1) < HALF
    for b in range(16):
        part[b, 0:16, :] = numer[b * 16 : b * 16 + 16]
        part[b, 16:24, :] = jnp.where(eight, wide[b * 16 : b * 16 + 8], wide[b * 16 + 8 : b * 16 + 16])

    for k in range(1, 16):
        x2 = lax.rem(col // 4 + k // 4, 4)
        y2 = lax.rem(lax.rem(col, 4) + k, 4)
        pltpu.make_async_remote_copy(
            src_ref=part.at[4 * x2 + y2], dst_ref=got.at[k], send_sem=r_ssem, recv_sem=r_rsem,
            device_id=(row, 4 * x2 + y2), device_id_type=MESH,
        ).start()
    result = part[col]
    pltpu.make_async_copy(got.at[pl.ds(1, 15)], got.at[pl.ds(1, 15)], r_rsem).wait()
    for k in range(1, 16):
        result = result + got[k]
    d8 = result[16:24] + RIDGE
    d8r = pltpu.roll(d8, 64, 1)
    out_ref[0:8, :] = result[0:8] / jnp.where(eight, d8, d8r)
    out_ref[8:16, :] = result[8:16] / jnp.where(eight, d8r, d8)

    pltpu.make_async_copy(send.at[pl.ds(0, 127)], send.at[pl.ds(0, 127)], d_ssem).wait()
    pltpu.make_async_copy(recvc.at[pl.ds(0, 127)], recvc.at[pl.ds(0, 127)], c_ssem).wait()
    pltpu.make_async_copy(part.at[pl.ds(0, 15)], part.at[pl.ds(0, 15)], r_ssem).wait()

    pltpu.make_async_copy(gcol.at[pl.ds(0, 112)], gcol.at[pl.ds(0, 112)], gs2_sem).wait()

    @pl.when(jnp.logical_not(g_mine))
    def _():
        pltpu.make_async_copy(gcol.at[pl.ds(0, 16)], gcol.at[pl.ds(0, 16)], gs_sem).wait()


def local_step(row_data, row_baseline, pair_table, lengths, model_vis, gains):
    any_space = pl.BlockSpec(memory_space=pl.ANY)
    vm = pltpu.VMEM
    dma = pltpu.SemaphoreType.DMA
    return pl.pallas_call(
        kernel,
        out_shape=jax.ShapeDtypeStruct((16, 128), F32),
        in_specs=[any_space] * 7,
        out_specs=pl.BlockSpec(memory_space=pltpu.VMEM),
        scratch_shapes=[
            vm((1, 128), F32), vm((ROWS, 128), BF16), vm((16, 128), I32), vm((2, SLOTS), I32), vm((32, 128), I32),
            vm((AR * AC, 128), BF16), vm((AR * AC, 128), F32),
            vm((32, 128), I32), pltpu.SMEM((32, 128), I32), vm((SLOTS, 128), F32),
            vm((144, ROWS), BF16), vm((ROWS, 128), I32),
            vm((DEVICES, HALF, 128), BF16), vm((DEVICES // 2, 1, 128), I32),
            vm((DEVICES, HALF, 128), BF16), vm((DEVICES, 1, 128), I32),
            vm((AC, 128), F32),
            vm((HALF, SLOTS), F32), vm((HALF, SLOTS), F32), vm((HALF, SLOTS), F32),
            vm((8, 128), I32), vm((144, 1024), BF16), vm((1024, 128), I32), vm((144, SLOTS), F32),
            vm((16, 24, 128), F32), vm((16, 24, 128), F32),
            vm((4, 144, 256), F32), vm((256, 128), BF16),
            dma((5,)), dma((8,)), dma, dma, dma, dma, dma, dma, dma((CHUNKS,)), dma, dma((CHUNKS,)), dma, dma,
        ],
        compiler_params=pltpu.CompilerParams(
            collective_id=0, has_side_effects=True, vmem_limit_bytes=60 * 2**20
        ),
    )(
        row_data,
        row_baseline.reshape(16, 128),
        pair_table.T,
        lengths.reshape(32, 128),
        model_vis.reshape(AR * AC, 128),
        gains,
        jnp.array([[32 * z + 16 * core + 4 * x + y for z, core, x, y in ORDER]], F32),
    )


def solution(mesh):
    rows = P(("arow", "acol"))
    placed = (
        P(("arow", "acol"), None),
        rows,
        P(("arow", "acol"), None),
        rows,
        P("arow", "acol", None),
        P(("arow", "acol"), None),
    )
    return jax.shard_map(
        local_step, mesh=mesh, in_specs=placed, out_specs=P(("arow", "acol"), None), check_vma=False
    )
```

```python
import itertools

import jax
import jax.numpy as jnp
from jax import lax
from jax.experimental import pallas as pl
from jax.experimental.pallas import tpu as pltpu
from jax.sharding import PartitionSpec as P

MESH = pl.DeviceIdType.MESH
RIDGE = 1.0
F32 = jnp.float32
BF16 = jnp.bfloat16
I32 = jnp.int32

ROWS = 2048
CAP = 64
SLOTS = 4096
AR = 256
AC = 128
HALF = 64
DEVICES = 128
CHUNKS = 8
LATE = 120
SELF = 127


def place():
    row = lax.axis_index("arow")
    col = lax.axis_index("acol")
    return row, col


def near_first():
    hops = (0, 1, 2, 1)

    def loads(offset):
        load = [0] * 6
        for axis, d in enumerate((offset[0], offset[2], offset[3])):
            if d != 3:
                load[2 * axis] += min(d, 1)
            if d > 1:
                load[2 * axis + 1] += 1
        return load

    left = [o for o in itertools.product(range(4), range(2), range(4), range(4)) if any(o)]
    order, total = [], [0] * 6
    while left:
        near = min(hops[o[0]] + hops[o[2]] + hops[o[3]] for o in left)

        def cost(o):
            after = [t + n for t, n in zip(total, loads(o))]
            return max(after), sum(a * a for a in after), o

        best = min((o for o in left if hops[o[0]] + hops[o[2]] + hops[o[3]] == near), key=cost)
        left.remove(best)
        order.append(best)
        total = [t + n for t, n in zip(total, loads(best))]
    return order + [(0, 0, 0, 0)]


ORDER = near_first()


def offset_of(owner):
    row, col = place()
    z = (owner // 32 - row // 2) & 3
    core = (owner // 16 - row) & 1
    x = (owner // 4 - col // 4) & 3
    return 32 * z + 16 * core + 4 * x + ((owner - col) & 3)


def each_tile(places, act):
    row, col = place()
    rows = [[2 * lax.rem(row // 2 + z, 4) + lax.rem(row + core, 2) for core in range(2)] for z in range(4)]
    xs = [4 * lax.rem(col // 4 + d, 4) for d in range(4)]
    ys = [lax.rem(col + d, 4) for d in range(4)]
    for pos in places:
        if pos != SELF:
            z, core, x, y = ORDER[pos]
            act(pos, (rows[z][core], xs[x] + ys[y]))


def iota(shape, dim):
    return lax.broadcasted_iota(I32, shape, dim)


def one_hot(match):
    return jnp.where(match, F32(1), F32(0)).astype(BF16)


def split_two(value):
    high = value.astype(BF16)
    return high, (value - high.astype(F32)).astype(BF16)


def kernel(
    x_hbm, rb_hbm, pair_hbm, len_hbm, m_hbm, g_hbm, order_hbm, out_ref,
    order_v, g_v, x_v, rb_v, pair_v, len_v, mb_v, mf_v, idx_v, idx_s, msel, xt, tgt,
    send, sendc, recv, recvc, gcol, cre, cim, den, codes, lhs, cb, acc,
    part, got, raw, gains_two,
    in_sem, m_sem, idx_sem, g_sem, gs_sem, g2_sem, gs2_sem, d_ssem, d_rsem, c_ssem, c_rsem, r_ssem, r_rsem,
):
    row, col = place()
    me = row * 16 + col

    loads = [
        pltpu.make_async_copy(rb_hbm, rb_v, in_sem.at[0]),
        pltpu.make_async_copy(pair_hbm, pair_v, in_sem.at[1]),
        pltpu.make_async_copy(x_hbm, x_v, in_sem.at[2]),
        pltpu.make_async_copy(len_hbm, len_v, in_sem.at[3]),
        pltpu.make_async_copy(order_hbm, order_v, in_sem.at[4]),
        pltpu.make_async_copy(g_hbm, g_v, in_sem.at[5]),
    ]
    for load in loads:
        load.start()
    m_loads = [
        pltpu.make_async_copy(m_hbm.at[pl.ds(j * 4096, 4096)], mb_v.at[pl.ds(j * 4096, 4096)], m_sem.at[j])
        for j in range(8)
    ]
    for load in m_loads:
        load.start()

    barrier = pltpu.get_barrier_semaphore()

    each_tile(
        range(DEVICES - 1, -1, -1),
        lambda pos, peer: pl.semaphore_signal(barrier, 1, device_id=peer, device_id_type=MESH),
    )

    loads[0].wait()
    slots = rb_v[...]
    owner = slots // SLOTS
    local = slots - owner * SLOTS + 1
    owner_t = offset_of(owner).astype(F32).T
    loads[4].wait()
    places = order_v[...]
    lower = one_hot(iota((256, 256), 0) > iota((256, 256), 1))
    spread = jnp.where(iota((256, 128), 0) < 128, F32(1), F32(CAP)).astype(BF16)
    lane = iota((256, 128), 1).astype(F32)
    before = jnp.zeros((1, 128), F32)
    for b in range(8):
        own = jnp.concatenate(
            [jnp.broadcast_to(owner_t[:, 2 * b + h : 2 * b + h + 1], (128, 128)) for h in range(2)], axis=0
        )
        hit = jnp.where(own == places, F32(1), F32(0))
        rows = slice(b * 256, b * 256 + 256)
        mf_v[rows, :] = hit
        msel[rows, :] = jnp.dot(lower, hit.astype(BF16), preferred_element_type=F32)
    for b in range(8):
        rows = slice(b * 256, b * 256 + 256)
        hit = mf_v[rows, :]
        within = msel[rows, :]
        two = jnp.concatenate([(hit * (within + before)).astype(BF16), (hit * lane).astype(BF16)], axis=1)
        tgt[rows, :] = jnp.dot(two, spread, preferred_element_type=F32).astype(I32)
        before = before + within[255:256, :] + hit[255:256, :]

    loads[1].wait()
    for k in range(32):
        p = pair_v[0:1, k * 128 : k * 128 + 128] - row * AR
        q = pair_v[1:2, k * 128 : k * 128 + 128] - col * AC
        idx_v[k : k + 1, :] = jnp.clip(p * AC + q, 0, AR * AC - 1)
    idx_copy = pltpu.make_async_copy(idx_v, idx_s, idx_sem)
    idx_copy.start()

    loads[2].wait()
    sub = iota((16, 128), 0)
    for b in range(16):
        xt[0:128, b * 128 : b * 128 + 128] = x_v[b * 128 : b * 128 + 128, :].T
        code = local[b : b + 1, :]
        high = code // 64
        digits = jnp.where(sub == 0, high, jnp.where(sub == 1, code - high * 64, 0))
        xt[128:144, b * 128 : b * 128 + 128] = digits.astype(F32).astype(BF16)

    acc[...] = jnp.zeros_like(acc)
    lhs[128:144, :] = jnp.ones((16, 1024), BF16)
    low_lanes = iota((HALF, 128), 1) < HALF

    def multiply(c, k):
        total = None
        for kb in range(8):
            rows = tgt[kb * 256 : kb * 256 + 256, :]
            hot = jnp.concatenate(
                [one_hot(rows == iota((256, 128), 1) + (c * 1024 + k * 256 + h * 128)) for h in range(2)], axis=1
            )
            term = jnp.dot(xt[:, kb * 256 : kb * 256 + 256], hot, preferred_element_type=F32)
            total = term if total is None else total + term
        raw[k] = total

    def arrange(c, k):
        for h in range(2):
            at = slice(h * 128, h * 128 + 128)
            re = raw[k, 0:64, at]
            im = pltpu.roll(raw[k, 64:128, at], 64, 1)
            send[c * 16 + k * 4 + 2 * h] = jnp.where(low_lanes, re, im).astype(BF16)
            send[c * 16 + k * 4 + 2 * h + 1] = jnp.where(low_lanes, im, re).astype(BF16)
            code = raw[k, 128:129, at] * 64.0 + raw[k, 129:130, at]
            sendc[c * 8 + k * 2 + h] = code.astype(I32) - 1

    def pack(c, beside):
        for k in range(4):
            multiply(c, k)
            beside(k)
            if k:
                arrange(c, k - 1)
        arrange(c, 3)

    def ship(c):
        def go(pos, peer):
            part_of = c + (pos >= LATE)
            pltpu.make_async_remote_copy(
                src_ref=sendc.at[pos // 2], dst_ref=recvc.at[pos],
                send_sem=c_ssem, recv_sem=c_rsem.at[part_of], device_id=peer, device_id_type=MESH,
            ).start()
            pltpu.make_async_remote_copy(
                src_ref=send.at[pos], dst_ref=recv.at[pos],
                send_sem=d_ssem, recv_sem=d_rsem.at[part_of], device_id=peer, device_id_type=MESH,
            ).start()

        each_tile(range(c * 16, c * 16 + 16), go)

    def widen(at, count):
        at = pl.ds(pl.multiple_of(at, 1024), count)
        mf_v[at, :] = mb_v[at, :].astype(F32)

    def wait_model(j):
        at = pl.ds(pl.multiple_of(j * 4096, 4096), 4096)
        pltpu.make_async_copy(m_hbm.at[at], mb_v.at[at], m_sem.at[j]).wait()

    pack(0, lambda k: None)
    pl.semaphore_wait(barrier, DEVICES - 1)

    g_row = lax.rem(me, 8)
    g_col = me // 8
    g_at = pl.ds(pl.multiple_of(g_row * 16, 16), 16)
    g_mine = jnp.logical_and(row == g_row, col == g_col)

    loads[5].wait()

    @pl.when(g_mine)
    def _():
        gcol[g_at, :] = g_v[...]

    @pl.when(jnp.logical_not(g_mine))
    def _():
        pltpu.make_async_remote_copy(
            src_ref=g_v, dst_ref=gcol.at[g_at], send_sem=gs_sem, recv_sem=g_sem,
            device_id=(g_row, g_col), device_id_type=MESH,
        ).start()

    ship(0)

    @pl.loop(1, CHUNKS)
    def _(c):
        wait_model(c)
        pack(c, lambda k: widen(c * 4096 + k * 1024, 1024))

        @pl.when(c == 4)
        def _():
            @pl.when(jnp.logical_not(g_mine))
            def _():
                pltpu.make_async_copy(gcol.at[pl.ds(0, 16)], gcol.at[pl.ds(0, 16)], g_sem).wait()

            my_gains = gcol.at[pl.ds(pl.multiple_of(row * 16, 16), 16)]
            for k in range(1, 8):
                pltpu.make_async_remote_copy(
                    src_ref=my_gains, dst_ref=my_gains, send_sem=gs2_sem, recv_sem=g2_sem,
                    device_id=(lax.rem(row + k, 8), col), device_id_type=MESH,
                ).start()

        for k in range(1, CHUNKS):
            @pl.when(c == k)
            def _():
                ship(k)

    recv[SELF] = send[SELF]
    recvc[SELF] = sendc[SELF // 2]
    wait_model(0)
    widen(0, 4096)
    idx_copy.wait()
    loads[3].wait()

    first_lanes = iota((1, 128), 1) < HALF

    def gather(block, u0, count):
        for u in range(u0, u0 + count):
            i = idx_s[block, u]
            msel[pl.ds(block * 128 + u, 1), :] = mf_v[pl.ds(i, 1), :]

    def slot_terms(block, gains_two):
        at = pl.ds(pl.multiple_of(block * 128, 128), 128)
        q = pair_v[1:2, at] - col * AC
        picked = jnp.dot(gains_two, one_hot(iota((128, 128), 0) == q), preferred_element_type=F32)
        g_re = picked[0:64] + picked[128:192]
        g_im = picked[64:128] + picked[192:256]
        model = msel[at, :].T
        m_re = model[0:64]
        m_im = model[64:128]
        c_re = m_re * g_re + m_im * g_im
        c_im = m_re * g_im - m_im * g_re
        w = len_v[pl.ds(block, 1), :].astype(F32)
        cre[:, at] = w * c_re
        cim[:, at] = w * c_im
        den[:, at] = w * (c_re * c_re + c_im * c_im)

    def arrived(j, senders):
        pltpu.make_async_copy(recv.at[pl.ds(0, senders)], recv.at[pl.ds(0, senders)], d_rsem.at[j]).wait()
        pltpu.make_async_copy(recvc.at[pl.ds(0, senders)], recvc.at[pl.ds(0, senders)], c_rsem.at[j]).wait()

    def add_chunk(first, pairs, beside):
        for s in range(pairs):
            a = recv[first + 2 * s].astype(F32)
            b = recv[first + 2 * s + 1].astype(F32)
            at = slice(s * 128, s * 128 + 128)
            lhs[0:64, at] = jnp.where(low_lanes, a, b).astype(BF16)
            lhs[64:128, at] = pltpu.roll(jnp.where(low_lanes, b, a), 64, 1).astype(BF16)
            codes[s : s + 1, :] = jnp.where(first_lanes, recvc[first + 2 * s], recvc[first + 2 * s + 1])
        codes_t = codes[...].astype(F32).T
        for s in range(pairs):
            cb[s * 128 : s * 128 + 128, :] = jnp.broadcast_to(codes_t[:, s : s + 1], (128, 128)).astype(I32)
        for nb in range(16):
            total = None
            for kb in range(pairs // 2):
                rows = cb[kb * 256 : kb * 256 + 256, :]
                hot = jnp.concatenate(
                    [one_hot(rows == iota((256, 128), 1) + (nb * 256 + h * 128)) for h in range(2)], axis=1
                )
                term = jnp.dot(lhs[:, kb * 256 : kb * 256 + 256], hot, preferred_element_type=F32)
                total = term if total is None else total + term
            acc[:, nb * 256 : nb * 256 + 256] += total
            beside(nb)

    @pl.loop(0, 4)
    def _(t):
        j = t + t // 3
        arrived(j, 16)
        add_chunk(j * 16, 8, lambda nb: gather(t * 8 + nb // 2, nb % 2 * 64, 64))

    @pl.loop(0, 2)
    def _(t):
        j = 5 - 2 * t
        arrived(j, 16)
        add_chunk(j * 16, 8, lambda nb: None)

    pltpu.make_async_copy(gcol.at[pl.ds(0, 112)], gcol.at[pl.ds(0, 112)], g2_sem).wait()
    gains_two[...] = jnp.concatenate(split_two(gcol[...].T), axis=0)

    def two_blocks(nb):
        slot_terms(2 * nb, gains_two[...])
        slot_terms(2 * nb + 1, gains_two[...])

    arrived(6, 16)
    add_chunk(96, 8, two_blocks)
    arrived(7, 8)
    add_chunk(112, 4, lambda nb: None)
    arrived(8, 7)
    add_chunk(LATE, 4, lambda nb: None)

    total = None
    for nb in range(16):
        at = slice(nb * 256, nb * 256 + 256)
        d_re = acc[0:64, at]
        d_im = acc[64:128, at]
        v = jnp.concatenate(
            [cre[:, at] * d_re - cim[:, at] * d_im, cre[:, at] * d_im + cim[:, at] * d_re, den[:, at] * acc[128:129, at]],
            axis=0,
        )
        both = jnp.concatenate(split_two(v), axis=0)
        p = pair_v[0:1, at] - row * AR
        hot = one_hot(iota((AR, 256), 0) == p)
        term = lax.dot_general(hot, both, (((1,), (1,)), ((), ())), preferred_element_type=F32)
        total = term if total is None else total + term
    numer = total[:, 0:128] + total[:, 192:320]
    denom = total[:, 128:192] + total[:, 320:384]
    wide = jnp.concatenate([denom, denom], axis=1)
    eight = iota((8, 128), 1) < HALF
    for b in range(16):
        part[b, 0:16, :] = numer[b * 16 : b * 16 + 16]
        part[b, 16:24, :] = jnp.where(eight, wide[b * 16 : b * 16 + 8], wide[b * 16 + 8 : b * 16 + 16])

    for k in range(1, 16):
        x2 = lax.rem(col // 4 + k // 4, 4)
        y2 = lax.rem(lax.rem(col, 4) + k, 4)
        pltpu.make_async_remote_copy(
            src_ref=part.at[4 * x2 + y2], dst_ref=got.at[k], send_sem=r_ssem, recv_sem=r_rsem,
            device_id=(row, 4 * x2 + y2), device_id_type=MESH,
        ).start()
    result = part[col]
    pltpu.make_async_copy(got.at[pl.ds(1, 15)], got.at[pl.ds(1, 15)], r_rsem).wait()
    for k in range(1, 16):
        result = result + got[k]
    d8 = result[16:24] + RIDGE
    d8r = pltpu.roll(d8, 64, 1)
    out_ref[0:8, :] = result[0:8] / jnp.where(eight, d8, d8r)
    out_ref[8:16, :] = result[8:16] / jnp.where(eight, d8r, d8)

    pltpu.make_async_copy(send.at[pl.ds(0, 127)], send.at[pl.ds(0, 127)], d_ssem).wait()
    pltpu.make_async_copy(recvc.at[pl.ds(0, 127)], recvc.at[pl.ds(0, 127)], c_ssem).wait()
    pltpu.make_async_copy(part.at[pl.ds(0, 15)], part.at[pl.ds(0, 15)], r_ssem).wait()

    pltpu.make_async_copy(gcol.at[pl.ds(0, 112)], gcol.at[pl.ds(0, 112)], gs2_sem).wait()

    @pl.when(jnp.logical_not(g_mine))
    def _():
        pltpu.make_async_copy(gcol.at[pl.ds(0, 16)], gcol.at[pl.ds(0, 16)], gs_sem).wait()


def local_step(row_data, row_baseline, pair_table, lengths, model_vis, gains):
    any_space = pl.BlockSpec(memory_space=pl.ANY)
    vm = pltpu.VMEM
    dma = pltpu.SemaphoreType.DMA
    return pl.pallas_call(
        kernel,
        out_shape=jax.ShapeDtypeStruct((16, 128), F32),
        in_specs=[any_space] * 7,
        out_specs=pl.BlockSpec(memory_space=pltpu.VMEM),
        scratch_shapes=[
            vm((1, 128), F32), vm((16, 128), F32), vm((ROWS, 128), BF16), vm((16, 128), I32), vm((2, SLOTS), I32), vm((32, 128), I32),
            vm((AR * AC, 128), BF16), vm((AR * AC, 128), F32),
            vm((32, 128), I32), pltpu.SMEM((32, 128), I32), vm((SLOTS, 128), F32),
            vm((144, ROWS), BF16), vm((ROWS, 128), I32),
            vm((DEVICES, HALF, 128), BF16), vm((DEVICES // 2, 1, 128), I32),
            vm((DEVICES, HALF, 128), BF16), vm((DEVICES, 1, 128), I32),
            vm((AC, 128), F32),
            vm((HALF, SLOTS), F32), vm((HALF, SLOTS), F32), vm((HALF, SLOTS), F32),
            vm((8, 128), I32), vm((144, 1024), BF16), vm((1024, 128), I32), vm((144, SLOTS), F32),
            vm((16, 24, 128), F32), vm((16, 24, 128), F32),
            vm((4, 144, 256), F32), vm((256, 128), BF16),
            dma((6,)), dma((8,)), dma, dma, dma, dma, dma, dma, dma((CHUNKS + 1,)), dma, dma((CHUNKS + 1,)), dma, dma,
        ],
        compiler_params=pltpu.CompilerParams(
            collective_id=0, has_side_effects=True, vmem_limit_bytes=60 * 2**20
        ),
    )(
        row_data,
        row_baseline.reshape(16, 128),
        pair_table.T,
        lengths.reshape(32, 128),
        model_vis.reshape(AR * AC, 128),
        gains,
        jnp.array([[32 * z + 16 * core + 4 * x + y for z, core, x, y in ORDER]], F32),
    )


def solution(mesh):
    rows = P(("arow", "acol"))
    placed = (
        P(("arow", "acol"), None),
        rows,
        P(("arow", "acol"), None),
        rows,
        P("arow", "acol", None),
        P(("arow", "acol"), None),
    )
    return jax.shard_map(
        local_step, mesh=mesh, in_specs=placed, out_specs=P(("arow", "acol"), None), check_vma=False
    )
```

```python
import itertools

import jax
import jax.numpy as jnp
from jax import lax
from jax.experimental import pallas as pl
from jax.experimental.pallas import tpu as pltpu
from jax.sharding import PartitionSpec as P

MESH = pl.DeviceIdType.MESH
RIDGE = 1.0
F32 = jnp.float32
BF16 = jnp.bfloat16
I32 = jnp.int32

ROWS = 2048
CAP = 64
SLOTS = 4096
AR = 256
AC = 128
HALF = 64
DEVICES = 128
CHUNKS = 8
LATE = 120
SELF = 127


def place():
    row = lax.axis_index("arow")
    col = lax.axis_index("acol")
    return row, col


def near_first():
    hops = (0, 1, 2, 1)

    def loads(offset):
        load = [0] * 6
        for axis, d in enumerate((offset[0], offset[2], offset[3])):
            if d != 3:
                load[2 * axis] += min(d, 1)
            if d > 1:
                load[2 * axis + 1] += 1
        return load

    left = [o for o in itertools.product(range(4), range(2), range(4), range(4)) if any(o)]
    order, total = [], [0] * 6
    while left:
        near = min(hops[o[0]] + hops[o[2]] + hops[o[3]] for o in left)

        def cost(o):
            after = [t + n for t, n in zip(total, loads(o))]
            return max(after), sum(a * a for a in after), o

        best = min((o for o in left if hops[o[0]] + hops[o[2]] + hops[o[3]] == near), key=cost)
        left.remove(best)
        order.append(best)
        total = [t + n for t, n in zip(total, loads(best))]
    return order + [(0, 0, 0, 0)]


ORDER = near_first()


def offset_of(owner):
    row, col = place()
    z = (owner // 32 - row // 2) & 3
    core = (owner // 16 - row) & 1
    x = (owner // 4 - col // 4) & 3
    return 32 * z + 16 * core + 4 * x + ((owner - col) & 3)


def each_tile(places, act):
    row, col = place()
    rows = [[2 * lax.rem(row // 2 + z, 4) + lax.rem(row + core, 2) for core in range(2)] for z in range(4)]
    xs = [4 * lax.rem(col // 4 + d, 4) for d in range(4)]
    ys = [lax.rem(col + d, 4) for d in range(4)]
    for pos in places:
        if pos != SELF:
            z, core, x, y = ORDER[pos]
            act(pos, (rows[z][core], xs[x] + ys[y]))


def iota(shape, dim):
    return lax.broadcasted_iota(I32, shape, dim)


def one_hot(match):
    return jnp.where(match, F32(1), F32(0)).astype(BF16)


def split_two(value):
    high = value.astype(BF16)
    return high, (value - high.astype(F32)).astype(BF16)


def kernel(
    x_hbm, rb_hbm, pair_hbm, len_hbm, m_hbm, g_hbm, order_hbm, out_ref,
    order_v, g_v, x_v, rb_v, pair_v, len_v, mb_v, mf_v, idx_v, idx_s, msel, xt, tgt,
    send, sendc, recv, recvc, gcol, cre, cim, den, codes, lhs, cb, acc,
    part, got, raw, gains_two,
    in_sem, m_sem, idx_sem, g_sem, gs_sem, g2_sem, gs2_sem, d_ssem, d_rsem, c_ssem, c_rsem, r_ssem, r_rsem,
):
    row, col = place()
    me = row * 16 + col

    loads = [
        pltpu.make_async_copy(rb_hbm, rb_v, in_sem.at[0]),
        pltpu.make_async_copy(pair_hbm, pair_v, in_sem.at[1]),
        pltpu.make_async_copy(x_hbm, x_v, in_sem.at[2]),
        pltpu.make_async_copy(len_hbm, len_v, in_sem.at[3]),
        pltpu.make_async_copy(order_hbm, order_v, in_sem.at[4]),
        pltpu.make_async_copy(g_hbm, g_v, in_sem.at[5]),
    ]
    for load in loads:
        load.start()
    m_loads = [
        pltpu.make_async_copy(m_hbm.at[pl.ds(j * 4096, 4096)], mb_v.at[pl.ds(j * 4096, 4096)], m_sem.at[j])
        for j in range(8)
    ]
    for load in m_loads:
        load.start()

    barrier = pltpu.get_barrier_semaphore()

    each_tile(
        range(DEVICES - 1, -1, -1),
        lambda pos, peer: pl.semaphore_signal(barrier, 1, device_id=peer, device_id_type=MESH),
    )

    loads[0].wait()
    slots = rb_v[...]
    owner = slots // SLOTS
    local = slots - owner * SLOTS + 1
    owner_t = offset_of(owner).astype(F32).T
    loads[4].wait()
    places = order_v[...]
    lower = one_hot(iota((256, 256), 0) > iota((256, 256), 1))
    spread = jnp.where(iota((256, 128), 0) < 128, F32(1), F32(CAP)).astype(BF16)
    lane = iota((256, 128), 1).astype(F32)
    before = jnp.zeros((1, 128), F32)
    for b in range(8):
        own = jnp.concatenate(
            [jnp.broadcast_to(owner_t[:, 2 * b + h : 2 * b + h + 1], (128, 128)) for h in range(2)], axis=0
        )
        hit = jnp.where(own == places, F32(1), F32(0))
        rows = slice(b * 256, b * 256 + 256)
        mf_v[rows, :] = hit
        msel[rows, :] = jnp.dot(lower, hit.astype(BF16), preferred_element_type=F32)
    for b in range(8):
        rows = slice(b * 256, b * 256 + 256)
        hit = mf_v[rows, :]
        within = msel[rows, :]
        two = jnp.concatenate([(hit * (within + before)).astype(BF16), (hit * lane).astype(BF16)], axis=1)
        tgt[rows, :] = jnp.dot(two, spread, preferred_element_type=F32).astype(I32)
        before = before + within[255:256, :] + hit[255:256, :]

    loads[1].wait()
    for k in range(32):
        p = pair_v[0:1, k * 128 : k * 128 + 128] - row * AR
        q = pair_v[1:2, k * 128 : k * 128 + 128] - col * AC
        idx_v[k : k + 1, :] = jnp.clip(p * AC + q, 0, AR * AC - 1)
    idx_copy = pltpu.make_async_copy(idx_v, idx_s, idx_sem)
    idx_copy.start()

    loads[2].wait()
    sub = iota((16, 128), 0)
    for b in range(16):
        xt[0:128, b * 128 : b * 128 + 128] = x_v[b * 128 : b * 128 + 128, :].T
        code = local[b : b + 1, :]
        high = code // 64
        digits = jnp.where(sub == 0, high, jnp.where(sub == 1, code - high * 64, 0))
        xt[128:144, b * 128 : b * 128 + 128] = digits.astype(F32).astype(BF16)

    acc[...] = jnp.zeros_like(acc)
    lhs[128:144, :] = jnp.ones((16, 1024), BF16)
    low_lanes = iota((HALF, 128), 1) < HALF

    def multiply(c, k):
        total = None
        for kb in range(8):
            rows = tgt[kb * 256 : kb * 256 + 256, :]
            hot = jnp.concatenate(
                [one_hot(rows == iota((256, 128), 1) + (c * 1024 + k * 256 + h * 128)) for h in range(2)], axis=1
            )
            term = jnp.dot(xt[:, kb * 256 : kb * 256 + 256], hot, preferred_element_type=F32)
            total = term if total is None else total + term
        raw[k] = total

    def arrange(c, k):
        for h in range(2):
            at = slice(h * 128, h * 128 + 128)
            re = raw[k, 0:64, at]
            im = pltpu.roll(raw[k, 64:128, at], 64, 1)
            send[c * 16 + k * 4 + 2 * h] = jnp.where(low_lanes, re, im).astype(BF16)
            send[c * 16 + k * 4 + 2 * h + 1] = jnp.where(low_lanes, im, re).astype(BF16)
            code = raw[k, 128:129, at] * 64.0 + raw[k, 129:130, at]
            sendc[c * 8 + k * 2 + h] = code.astype(I32) - 1

    def pack(c, beside):
        for k in range(4):
            multiply(c, k)
            beside(k)
            if k:
                arrange(c, k - 1)
        arrange(c, 3)

    def ship(c):
        def go(pos, peer):
            part_of = c + (pos >= LATE)
            pltpu.make_async_remote_copy(
                src_ref=sendc.at[pos // 2], dst_ref=recvc.at[pos],
                send_sem=c_ssem, recv_sem=c_rsem.at[part_of], device_id=peer, device_id_type=MESH,
            ).start()
            pltpu.make_async_remote_copy(
                src_ref=send.at[pos], dst_ref=recv.at[pos],
                send_sem=d_ssem, recv_sem=d_rsem.at[part_of], device_id=peer, device_id_type=MESH,
            ).start()

        each_tile(range(c * 16, c * 16 + 16), go)

    def widen(at, count):
        at = pl.ds(pl.multiple_of(at, 1024), count)
        mf_v[at, :] = mb_v[at, :].astype(F32)

    def wait_model(j):
        at = pl.ds(pl.multiple_of(j * 4096, 4096), 4096)
        pltpu.make_async_copy(m_hbm.at[at], mb_v.at[at], m_sem.at[j]).wait()

    pack(0, lambda k: None)
    pl.semaphore_wait(barrier, DEVICES - 1)

    g_row = lax.rem(me, 8)
    g_col = me // 8
    g_at = pl.ds(pl.multiple_of(g_row * 16, 16), 16)
    g_mine = jnp.logical_and(row == g_row, col == g_col)

    loads[5].wait()

    @pl.when(g_mine)
    def _():
        gcol[g_at, :] = g_v[...]

    @pl.when(jnp.logical_not(g_mine))
    def _():
        pltpu.make_async_remote_copy(
            src_ref=g_v, dst_ref=gcol.at[g_at], send_sem=gs_sem, recv_sem=g_sem,
            device_id=(g_row, g_col), device_id_type=MESH,
        ).start()

    ship(0)

    @pl.loop(1, CHUNKS)
    def _(c):
        wait_model(c)
        pack(c, lambda k: widen(c * 4096 + k * 1024, 1024))

        @pl.when(c == 4)
        def _():
            @pl.when(jnp.logical_not(g_mine))
            def _():
                pltpu.make_async_copy(gcol.at[pl.ds(0, 16)], gcol.at[pl.ds(0, 16)], g_sem).wait()

            my_gains = gcol.at[pl.ds(pl.multiple_of(row * 16, 16), 16)]
            for k in range(1, 8):
                pltpu.make_async_remote_copy(
                    src_ref=my_gains, dst_ref=my_gains, send_sem=gs2_sem, recv_sem=g2_sem,
                    device_id=(lax.rem(row + k, 8), col), device_id_type=MESH,
                ).start()

        for k in range(1, CHUNKS):
            @pl.when(c == k)
            def _():
                ship(k)

    recv[SELF] = send[SELF]
    recvc[SELF] = sendc[SELF // 2]
    wait_model(0)
    widen(0, 4096)
    idx_copy.wait()
    loads[3].wait()

    first_lanes = iota((1, 128), 1) < HALF

    def gather(block, u0, count):
        for u in range(u0, u0 + count):
            i = idx_s[block, u]
            msel[pl.ds(block * 128 + u, 1), :] = mf_v[pl.ds(i, 1), :]

    def slot_terms(block, gains_two):
        at = pl.ds(pl.multiple_of(block * 128, 128), 128)
        q = pair_v[1:2, at] - col * AC
        picked = jnp.dot(gains_two, one_hot(iota((128, 128), 0) == q), preferred_element_type=F32)
        g_re = picked[0:64] + picked[128:192]
        g_im = picked[64:128] + picked[192:256]
        model = msel[at, :].T
        m_re = model[0:64]
        m_im = model[64:128]
        c_re = m_re * g_re + m_im * g_im
        c_im = m_re * g_im - m_im * g_re
        w = len_v[pl.ds(block, 1), :].astype(F32)
        cre[:, at] = w * c_re
        cim[:, at] = w * c_im
        den[:, at] = w * (c_re * c_re + c_im * c_im)

    def arrived(j, senders):
        pltpu.make_async_copy(recv.at[pl.ds(0, senders)], recv.at[pl.ds(0, senders)], d_rsem.at[j]).wait()
        pltpu.make_async_copy(recvc.at[pl.ds(0, senders)], recvc.at[pl.ds(0, senders)], c_rsem.at[j]).wait()

    def add_chunk(first, pairs, beside):
        for s in range(pairs):
            a = recv[first + 2 * s].astype(F32)
            b = recv[first + 2 * s + 1].astype(F32)
            at = slice(s * 128, s * 128 + 128)
            lhs[0:64, at] = jnp.where(low_lanes, a, b).astype(BF16)
            lhs[64:128, at] = pltpu.roll(jnp.where(low_lanes, b, a), 64, 1).astype(BF16)
            codes[s : s + 1, :] = jnp.where(first_lanes, recvc[first + 2 * s], recvc[first + 2 * s + 1])
        codes_t = codes[...].astype(F32).T
        for s in range(pairs):
            cb[s * 128 : s * 128 + 128, :] = jnp.broadcast_to(codes_t[:, s : s + 1], (128, 128)).astype(I32)
        for nb in range(16):
            total = None
            for kb in range(pairs // 2):
                rows = cb[kb * 256 : kb * 256 + 256, :]
                hot = jnp.concatenate(
                    [one_hot(rows == iota((256, 128), 1) + (nb * 256 + h * 128)) for h in range(2)], axis=1
                )
                term = jnp.dot(lhs[:, kb * 256 : kb * 256 + 256], hot, preferred_element_type=F32)
                total = term if total is None else total + term
            acc[:, nb * 256 : nb * 256 + 256] += total
            beside(nb)

    @pl.loop(0, 4)
    def _(t):
        j = t + t // 3
        arrived(j, 16)
        add_chunk(j * 16, 8, lambda nb: gather(t * 8 + nb // 2, nb % 2 * 64, 64))

    @pl.loop(0, 2)
    def _(t):
        j = 5 - 2 * t
        arrived(j, 16)
        add_chunk(j * 16, 8, lambda nb: None)

    arrived(6, 16)
    add_chunk(96, 8, lambda nb: None)
    pltpu.make_async_copy(gcol.at[pl.ds(0, 112)], gcol.at[pl.ds(0, 112)], g2_sem).wait()
    gains_two[...] = jnp.concatenate(split_two(gcol[...].T), axis=0)

    def two_blocks(nb):
        slot_terms(2 * nb, gains_two[...])
        slot_terms(2 * nb + 1, gains_two[...])

    arrived(7, 8)
    add_chunk(112, 4, two_blocks)
    arrived(8, 7)
    add_chunk(LATE, 4, lambda nb: None)

    total = None
    for nb in range(16):
        at = slice(nb * 256, nb * 256 + 256)
        d_re = acc[0:64, at]
        d_im = acc[64:128, at]
        v = jnp.concatenate(
            [cre[:, at] * d_re - cim[:, at] * d_im, cre[:, at] * d_im + cim[:, at] * d_re, den[:, at] * acc[128:129, at]],
            axis=0,
        )
        both = jnp.concatenate(split_two(v), axis=0)
        p = pair_v[0:1, at] - row * AR
        hot = one_hot(iota((AR, 256), 0) == p)
        term = lax.dot_general(hot, both, (((1,), (1,)), ((), ())), preferred_element_type=F32)
        total = term if total is None else total + term
    numer = total[:, 0:128] + total[:, 192:320]
    denom = total[:, 128:192] + total[:, 320:384]
    wide = jnp.concatenate([denom, denom], axis=1)
    eight = iota((8, 128), 1) < HALF
    for b in range(16):
        part[b, 0:16, :] = numer[b * 16 : b * 16 + 16]
        part[b, 16:24, :] = jnp.where(eight, wide[b * 16 : b * 16 + 8], wide[b * 16 + 8 : b * 16 + 16])

    hops = (0, 1, 2, 1)
    for k in sorted(range(1, 16), key=lambda k: -hops[k // 4] - hops[k % 4]):
        x2 = lax.rem(col // 4 + k // 4, 4)
        y2 = lax.rem(lax.rem(col, 4) + k, 4)
        pltpu.make_async_remote_copy(
            src_ref=part.at[4 * x2 + y2], dst_ref=got.at[k], send_sem=r_ssem, recv_sem=r_rsem,
            device_id=(row, 4 * x2 + y2), device_id_type=MESH,
        ).start()
    result = part[col]
    pltpu.make_async_copy(got.at[pl.ds(1, 15)], got.at[pl.ds(1, 15)], r_rsem).wait()
    for k in range(1, 16):
        result = result + got[k]
    d8 = result[16:24] + RIDGE
    d8r = pltpu.roll(d8, 64, 1)
    out_ref[0:8, :] = result[0:8] / jnp.where(eight, d8, d8r)
    out_ref[8:16, :] = result[8:16] / jnp.where(eight, d8r, d8)

    pltpu.make_async_copy(send.at[pl.ds(0, 127)], send.at[pl.ds(0, 127)], d_ssem).wait()
    pltpu.make_async_copy(recvc.at[pl.ds(0, 127)], recvc.at[pl.ds(0, 127)], c_ssem).wait()
    pltpu.make_async_copy(part.at[pl.ds(0, 15)], part.at[pl.ds(0, 15)], r_ssem).wait()

    pltpu.make_async_copy(gcol.at[pl.ds(0, 112)], gcol.at[pl.ds(0, 112)], gs2_sem).wait()

    @pl.when(jnp.logical_not(g_mine))
    def _():
        pltpu.make_async_copy(gcol.at[pl.ds(0, 16)], gcol.at[pl.ds(0, 16)], gs_sem).wait()


def local_step(row_data, row_baseline, pair_table, lengths, model_vis, gains):
    any_space = pl.BlockSpec(memory_space=pl.ANY)
    vm = pltpu.VMEM
    dma = pltpu.SemaphoreType.DMA
    return pl.pallas_call(
        kernel,
        out_shape=jax.ShapeDtypeStruct((16, 128), F32),
        in_specs=[any_space] * 7,
        out_specs=pl.BlockSpec(memory_space=pltpu.VMEM),
        scratch_shapes=[
            vm((1, 128), F32), vm((16, 128), F32), vm((ROWS, 128), BF16), vm((16, 128), I32), vm((2, SLOTS), I32), vm((32, 128), I32),
            vm((AR * AC, 128), BF16), vm((AR * AC, 128), F32),
            vm((32, 128), I32), pltpu.SMEM((32, 128), I32), vm((SLOTS, 128), F32),
            vm((144, ROWS), BF16), vm((ROWS, 128), I32),
            vm((DEVICES, HALF, 128), BF16), vm((DEVICES // 2, 1, 128), I32),
            vm((DEVICES, HALF, 128), BF16), vm((DEVICES, 1, 128), I32),
            vm((AC, 128), F32),
            vm((HALF, SLOTS), F32), vm((HALF, SLOTS), F32), vm((HALF, SLOTS), F32),
            vm((8, 128), I32), vm((144, 1024), BF16), vm((1024, 128), I32), vm((144, SLOTS), F32),
            vm((16, 24, 128), F32), vm((16, 24, 128), F32),
            vm((4, 144, 256), F32), vm((256, 128), BF16),
            dma((6,)), dma((8,)), dma, dma, dma, dma, dma, dma, dma((CHUNKS + 1,)), dma, dma((CHUNKS + 1,)), dma, dma,
        ],
        compiler_params=pltpu.CompilerParams(
            collective_id=0, has_side_effects=True, vmem_limit_bytes=60 * 2**20
        ),
    )(
        row_data,
        row_baseline.reshape(16, 128),
        pair_table.T,
        lengths.reshape(32, 128),
        model_vis.reshape(AR * AC, 128),
        gains,
        jnp.array([[32 * z + 16 * core + 4 * x + y for z, core, x, y in ORDER]], F32),
    )


def solution(mesh):
    rows = P(("arow", "acol"))
    placed = (
        P(("arow", "acol"), None),
        rows,
        P(("arow", "acol"), None),
        rows,
        P("arow", "acol", None),
        P(("arow", "acol"), None),
    )
    return jax.shard_map(
        local_step, mesh=mesh, in_specs=placed, out_specs=P(("arow", "acol"), None), check_vma=False
    )
```

```python
import itertools

import jax
import jax.numpy as jnp
from jax import lax
from jax.experimental import pallas as pl
from jax.experimental.pallas import tpu as pltpu
from jax.sharding import PartitionSpec as P

MESH = pl.DeviceIdType.MESH
RIDGE = 1.0
F32 = jnp.float32
BF16 = jnp.bfloat16
I32 = jnp.int32

ROWS = 2048
CAP = 64
SLOTS = 4096
AR = 256
AC = 128
HALF = 64
DEVICES = 128
CHUNKS = 8
LATE = 124
SELF = 127


def place():
    row = lax.axis_index("arow")
    col = lax.axis_index("acol")
    return row, col


def near_first():
    hops = (0, 1, 2, 1)

    def loads(offset):
        load = [0] * 6
        for axis, d in enumerate((offset[0], offset[2], offset[3])):
            if d != 3:
                load[2 * axis] += min(d, 1)
            if d > 1:
                load[2 * axis + 1] += 1
        return load

    left = [o for o in itertools.product(range(4), range(2), range(4), range(4)) if any(o)]
    order, total = [], [0] * 6
    while left:
        near = min(hops[o[0]] + hops[o[2]] + hops[o[3]] for o in left)

        def cost(o):
            after = [t + n for t, n in zip(total, loads(o))]
            return max(after), sum(a * a for a in after), o

        best = min((o for o in left if hops[o[0]] + hops[o[2]] + hops[o[3]] == near), key=cost)
        left.remove(best)
        order.append(best)
        total = [t + n for t, n in zip(total, loads(best))]
    return order + [(0, 0, 0, 0)]


ORDER = near_first()


def offset_of(owner):
    row, col = place()
    z = (owner // 32 - row // 2) & 3
    core = (owner // 16 - row) & 1
    x = (owner // 4 - col // 4) & 3
    return 32 * z + 16 * core + 4 * x + ((owner - col) & 3)


def each_tile(places, act):
    row, col = place()
    rows = [[2 * lax.rem(row // 2 + z, 4) + lax.rem(row + core, 2) for core in range(2)] for z in range(4)]
    xs = [4 * lax.rem(col // 4 + d, 4) for d in range(4)]
    ys = [lax.rem(col + d, 4) for d in range(4)]
    for pos in places:
        if pos != SELF:
            z, core, x, y = ORDER[pos]
            act(pos, (rows[z][core], xs[x] + ys[y]))


def iota(shape, dim):
    return lax.broadcasted_iota(I32, shape, dim)


def one_hot(match):
    return jnp.where(match, F32(1), F32(0)).astype(BF16)


def split_two(value):
    high = value.astype(BF16)
    return high, (value - high.astype(F32)).astype(BF16)


def kernel(
    x_hbm, rb_hbm, pair_hbm, len_hbm, m_hbm, g_hbm, order_hbm, out_ref,
    order_v, g_v, x_v, rb_v, pair_v, len_v, mb_v, mf_v, idx_v, idx_s, msel, xt, tgt,
    send, sendc, recv, recvc, gcol, cre, cim, den, codes, lhs, cb, acc,
    part, got, raw, gains_two,
    in_sem, m_sem, idx_sem, g_sem, gs_sem, g2_sem, gs2_sem, d_ssem, d_rsem, c_ssem, c_rsem, r_ssem, r_rsem,
):
    row, col = place()
    me = row * 16 + col

    loads = [
        pltpu.make_async_copy(rb_hbm, rb_v, in_sem.at[0]),
        pltpu.make_async_copy(pair_hbm, pair_v, in_sem.at[1]),
        pltpu.make_async_copy(x_hbm, x_v, in_sem.at[2]),
        pltpu.make_async_copy(len_hbm, len_v, in_sem.at[3]),
        pltpu.make_async_copy(order_hbm, order_v, in_sem.at[4]),
        pltpu.make_async_copy(g_hbm, g_v, in_sem.at[5]),
    ]
    for load in loads:
        load.start()
    m_loads = [
        pltpu.make_async_copy(m_hbm.at[pl.ds(j * 4096, 4096)], mb_v.at[pl.ds(j * 4096, 4096)], m_sem.at[j])
        for j in range(8)
    ]
    for load in m_loads:
        load.start()

    barrier = pltpu.get_barrier_semaphore()

    each_tile(
        range(DEVICES - 1, -1, -1),
        lambda pos, peer: pl.semaphore_signal(barrier, 1, device_id=peer, device_id_type=MESH),
    )

    loads[0].wait()
    slots = rb_v[...]
    owner = slots // SLOTS
    local = slots - owner * SLOTS + 1
    owner_t = offset_of(owner).astype(F32).T
    loads[4].wait()
    places = order_v[...]
    lower = one_hot(iota((256, 256), 0) > iota((256, 256), 1))
    spread = jnp.where(iota((256, 128), 0) < 128, F32(1), F32(CAP)).astype(BF16)
    lane = iota((256, 128), 1).astype(F32)
    before = jnp.zeros((1, 128), F32)
    for b in range(8):
        own = jnp.concatenate(
            [jnp.broadcast_to(owner_t[:, 2 * b + h : 2 * b + h + 1], (128, 128)) for h in range(2)], axis=0
        )
        hit = jnp.where(own == places, F32(1), F32(0))
        rows = slice(b * 256, b * 256 + 256)
        mf_v[rows, :] = hit
        msel[rows, :] = jnp.dot(lower, hit.astype(BF16), preferred_element_type=F32)
    for b in range(8):
        rows = slice(b * 256, b * 256 + 256)
        hit = mf_v[rows, :]
        within = msel[rows, :]
        two = jnp.concatenate([(hit * (within + before)).astype(BF16), (hit * lane).astype(BF16)], axis=1)
        tgt[rows, :] = jnp.dot(two, spread, preferred_element_type=F32).astype(I32)
        before = before + within[255:256, :] + hit[255:256, :]

    loads[1].wait()
    for k in range(32):
        p = pair_v[0:1, k * 128 : k * 128 + 128] - row * AR
        q = pair_v[1:2, k * 128 : k * 128 + 128] - col * AC
        idx_v[k : k + 1, :] = jnp.clip(p * AC + q, 0, AR * AC - 1)
    idx_copy = pltpu.make_async_copy(idx_v, idx_s, idx_sem)
    idx_copy.start()

    loads[2].wait()
    sub = iota((16, 128), 0)
    for b in range(16):
        xt[0:128, b * 128 : b * 128 + 128] = x_v[b * 128 : b * 128 + 128, :].T
        code = local[b : b + 1, :]
        high = code // 64
        digits = jnp.where(sub == 0, high, jnp.where(sub == 1, code - high * 64, 0))
        xt[128:144, b * 128 : b * 128 + 128] = digits.astype(F32).astype(BF16)

    acc[...] = jnp.zeros_like(acc)
    lhs[128:144, :] = jnp.ones((16, 1024), BF16)
    low_lanes = iota((HALF, 128), 1) < HALF

    def multiply(c, k):
        total = None
        for kb in range(8):
            rows = tgt[kb * 256 : kb * 256 + 256, :]
            hot = jnp.concatenate(
                [one_hot(rows == iota((256, 128), 1) + (c * 1024 + k * 256 + h * 128)) for h in range(2)], axis=1
            )
            term = jnp.dot(xt[:, kb * 256 : kb * 256 + 256], hot, preferred_element_type=F32)
            total = term if total is None else total + term
        raw[k] = total

    def arrange(c, k):
        for h in range(2):
            at = slice(h * 128, h * 128 + 128)
            re = raw[k, 0:64, at]
            im = pltpu.roll(raw[k, 64:128, at], 64, 1)
            send[c * 16 + k * 4 + 2 * h] = jnp.where(low_lanes, re, im).astype(BF16)
            send[c * 16 + k * 4 + 2 * h + 1] = jnp.where(low_lanes, im, re).astype(BF16)
            code = raw[k, 128:129, at] * 64.0 + raw[k, 129:130, at]
            sendc[c * 8 + k * 2 + h] = code.astype(I32) - 1

    def pack(c, beside):
        for k in range(4):
            multiply(c, k)
            beside(k)
            if k:
                arrange(c, k - 1)
        arrange(c, 3)

    def ship(c):
        def go(pos, peer):
            part_of = c + (pos >= LATE)
            pltpu.make_async_remote_copy(
                src_ref=sendc.at[pos // 2], dst_ref=recvc.at[pos],
                send_sem=c_ssem, recv_sem=c_rsem.at[part_of], device_id=peer, device_id_type=MESH,
            ).start()
            pltpu.make_async_remote_copy(
                src_ref=send.at[pos], dst_ref=recv.at[pos],
                send_sem=d_ssem, recv_sem=d_rsem.at[part_of], device_id=peer, device_id_type=MESH,
            ).start()

        each_tile(range(c * 16, c * 16 + 16), go)

    def widen(at, count):
        at = pl.ds(pl.multiple_of(at, 1024), count)
        mf_v[at, :] = mb_v[at, :].astype(F32)

    def wait_model(j):
        at = pl.ds(pl.multiple_of(j * 4096, 4096), 4096)
        pltpu.make_async_copy(m_hbm.at[at], mb_v.at[at], m_sem.at[j]).wait()

    pack(0, lambda k: None)
    pl.semaphore_wait(barrier, DEVICES - 1)

    g_row = lax.rem(me, 8)
    g_col = me // 8
    g_at = pl.ds(pl.multiple_of(g_row * 16, 16), 16)
    g_mine = jnp.logical_and(row == g_row, col == g_col)

    loads[5].wait()

    @pl.when(g_mine)
    def _():
        gcol[g_at, :] = g_v[...]

    @pl.when(jnp.logical_not(g_mine))
    def _():
        pltpu.make_async_remote_copy(
            src_ref=g_v, dst_ref=gcol.at[g_at], send_sem=gs_sem, recv_sem=g_sem,
            device_id=(g_row, g_col), device_id_type=MESH,
        ).start()

    ship(0)

    @pl.loop(1, CHUNKS)
    def _(c):
        wait_model(c)
        pack(c, lambda k: widen(c * 4096 + k * 1024, 1024))

        @pl.when(c == 4)
        def _():
            @pl.when(jnp.logical_not(g_mine))
            def _():
                pltpu.make_async_copy(gcol.at[pl.ds(0, 16)], gcol.at[pl.ds(0, 16)], g_sem).wait()

            my_gains = gcol.at[pl.ds(pl.multiple_of(row * 16, 16), 16)]
            for k in range(1, 8):
                pltpu.make_async_remote_copy(
                    src_ref=my_gains, dst_ref=my_gains, send_sem=gs2_sem, recv_sem=g2_sem,
                    device_id=(lax.rem(row + k, 8), col), device_id_type=MESH,
                ).start()

        for k in range(1, CHUNKS):
            @pl.when(c == k)
            def _():
                ship(k)

    recv[SELF] = send[SELF]
    recvc[SELF] = sendc[SELF // 2]
    wait_model(0)
    widen(0, 4096)
    idx_copy.wait()
    loads[3].wait()

    first_lanes = iota((1, 128), 1) < HALF

    def gather(block, u0, count):
        for u in range(u0, u0 + count):
            i = idx_s[block, u]
            msel[pl.ds(block * 128 + u, 1), :] = mf_v[pl.ds(i, 1), :]

    def slot_terms(block, gains_two):
        at = pl.ds(pl.multiple_of(block * 128, 128), 128)
        q = pair_v[1:2, at] - col * AC
        picked = jnp.dot(gains_two, one_hot(iota((128, 128), 0) == q), preferred_element_type=F32)
        g_re = picked[0:64] + picked[128:192]
        g_im = picked[64:128] + picked[192:256]
        model = msel[at, :].T
        m_re = model[0:64]
        m_im = model[64:128]
        c_re = m_re * g_re + m_im * g_im
        c_im = m_re * g_im - m_im * g_re
        w = len_v[pl.ds(block, 1), :].astype(F32)
        cre[:, at] = w * c_re
        cim[:, at] = w * c_im
        den[:, at] = w * (c_re * c_re + c_im * c_im)

    def arrived(j, senders):
        pltpu.make_async_copy(recv.at[pl.ds(0, senders)], recv.at[pl.ds(0, senders)], d_rsem.at[j]).wait()
        pltpu.make_async_copy(recvc.at[pl.ds(0, senders)], recvc.at[pl.ds(0, senders)], c_rsem.at[j]).wait()

    def add_chunk(first, pairs, beside):
        for s in range(pairs):
            a = recv[first + 2 * s].astype(F32)
            b = recv[first + 2 * s + 1].astype(F32)
            at = slice(s * 128, s * 128 + 128)
            lhs[0:64, at] = jnp.where(low_lanes, a, b).astype(BF16)
            lhs[64:128, at] = pltpu.roll(jnp.where(low_lanes, b, a), 64, 1).astype(BF16)
            codes[s : s + 1, :] = jnp.where(first_lanes, recvc[first + 2 * s], recvc[first + 2 * s + 1])
        codes_t = codes[...].astype(F32).T
        for s in range(pairs):
            cb[s * 128 : s * 128 + 128, :] = jnp.broadcast_to(codes_t[:, s : s + 1], (128, 128)).astype(I32)
        for nb in range(16):
            total = None
            for kb in range(pairs // 2):
                rows = cb[kb * 256 : kb * 256 + 256, :]
                hot = jnp.concatenate(
                    [one_hot(rows == iota((256, 128), 1) + (nb * 256 + h * 128)) for h in range(2)], axis=1
                )
                term = jnp.dot(lhs[:, kb * 256 : kb * 256 + 256], hot, preferred_element_type=F32)
                total = term if total is None else total + term
            acc[:, nb * 256 : nb * 256 + 256] += total
            beside(nb)

    @pl.loop(0, 4)
    def _(t):
        j = t + t // 3
        arrived(j, 16)
        add_chunk(j * 16, 8, lambda nb: gather(t * 8 + nb // 2, nb % 2 * 64, 64))

    @pl.loop(0, 2)
    def _(t):
        j = 5 - 2 * t
        arrived(j, 16)
        add_chunk(j * 16, 8, lambda nb: None)

    arrived(6, 16)
    add_chunk(96, 8, lambda nb: None)
    pltpu.make_async_copy(gcol.at[pl.ds(0, 112)], gcol.at[pl.ds(0, 112)], g2_sem).wait()
    gains_two[...] = jnp.concatenate(split_two(gcol[...].T), axis=0)

    def two_blocks(nb):
        slot_terms(2 * nb, gains_two[...])
        slot_terms(2 * nb + 1, gains_two[...])

    arrived(7, 12)
    add_chunk(112, 6, two_blocks)
    arrived(8, 3)
    add_chunk(LATE, 2, lambda nb: None)

    total = None
    for nb in range(16):
        at = slice(nb * 256, nb * 256 + 256)
        d_re = acc[0:64, at]
        d_im = acc[64:128, at]
        v = jnp.concatenate(
            [cre[:, at] * d_re - cim[:, at] * d_im, cre[:, at] * d_im + cim[:, at] * d_re, den[:, at] * acc[128:129, at]],
            axis=0,
        )
        both = jnp.concatenate(split_two(v), axis=0)
        p = pair_v[0:1, at] - row * AR
        hot = one_hot(iota((AR, 256), 0) == p)
        term = lax.dot_general(hot, both, (((1,), (1,)), ((), ())), preferred_element_type=F32)
        total = term if total is None else total + term
    numer = total[:, 0:128] + total[:, 192:320]
    denom = total[:, 128:192] + total[:, 320:384]
    wide = jnp.concatenate([denom, denom], axis=1)
    eight = iota((8, 128), 1) < HALF
    for b in range(16):
        part[b, 0:16, :] = numer[b * 16 : b * 16 + 16]
        part[b, 16:24, :] = jnp.where(eight, wide[b * 16 : b * 16 + 8], wide[b * 16 + 8 : b * 16 + 16])

    hops = (0, 1, 2, 1)
    for k in sorted(range(1, 16), key=lambda k: -hops[k // 4] - hops[k % 4]):
        x2 = lax.rem(col // 4 + k // 4, 4)
        y2 = lax.rem(lax.rem(col, 4) + k, 4)
        pltpu.make_async_remote_copy(
            src_ref=part.at[4 * x2 + y2], dst_ref=got.at[k], send_sem=r_ssem, recv_sem=r_rsem,
            device_id=(row, 4 * x2 + y2), device_id_type=MESH,
        ).start()
    result = part[col]
    pltpu.make_async_copy(got.at[pl.ds(1, 15)], got.at[pl.ds(1, 15)], r_rsem).wait()
    for k in range(1, 16):
        result = result + got[k]
    d8 = result[16:24] + RIDGE
    d8r = pltpu.roll(d8, 64, 1)
    out_ref[0:8, :] = result[0:8] / jnp.where(eight, d8, d8r)
    out_ref[8:16, :] = result[8:16] / jnp.where(eight, d8r, d8)

    pltpu.make_async_copy(send.at[pl.ds(0, 127)], send.at[pl.ds(0, 127)], d_ssem).wait()
    pltpu.make_async_copy(recvc.at[pl.ds(0, 127)], recvc.at[pl.ds(0, 127)], c_ssem).wait()
    pltpu.make_async_copy(part.at[pl.ds(0, 15)], part.at[pl.ds(0, 15)], r_ssem).wait()

    pltpu.make_async_copy(gcol.at[pl.ds(0, 112)], gcol.at[pl.ds(0, 112)], gs2_sem).wait()

    @pl.when(jnp.logical_not(g_mine))
    def _():
        pltpu.make_async_copy(gcol.at[pl.ds(0, 16)], gcol.at[pl.ds(0, 16)], gs_sem).wait()


def local_step(row_data, row_baseline, pair_table, lengths, model_vis, gains):
    any_space = pl.BlockSpec(memory_space=pl.ANY)
    vm = pltpu.VMEM
    dma = pltpu.SemaphoreType.DMA
    return pl.pallas_call(
        kernel,
        out_shape=jax.ShapeDtypeStruct((16, 128), F32),
        in_specs=[any_space] * 7,
        out_specs=pl.BlockSpec(memory_space=pltpu.VMEM),
        scratch_shapes=[
            vm((1, 128), F32), vm((16, 128), F32), vm((ROWS, 128), BF16), vm((16, 128), I32), vm((2, SLOTS), I32), vm((32, 128), I32),
            vm((AR * AC, 128), BF16), vm((AR * AC, 128), F32),
            vm((32, 128), I32), pltpu.SMEM((32, 128), I32), vm((SLOTS, 128), F32),
            vm((144, ROWS), BF16), vm((ROWS, 128), I32),
            vm((DEVICES, HALF, 128), BF16), vm((DEVICES // 2, 1, 128), I32),
            vm((DEVICES, HALF, 128), BF16), vm((DEVICES, 1, 128), I32),
            vm((AC, 128), F32),
            vm((HALF, SLOTS), F32), vm((HALF, SLOTS), F32), vm((HALF, SLOTS), F32),
            vm((8, 128), I32), vm((144, 1024), BF16), vm((1024, 128), I32), vm((144, SLOTS), F32),
            vm((16, 24, 128), F32), vm((16, 24, 128), F32),
            vm((4, 144, 256), F32), vm((256, 128), BF16),
            dma((6,)), dma((8,)), dma, dma, dma, dma, dma, dma, dma((CHUNKS + 1,)), dma, dma((CHUNKS + 1,)), dma, dma,
        ],
        compiler_params=pltpu.CompilerParams(
            collective_id=0, has_side_effects=True, vmem_limit_bytes=60 * 2**20
        ),
    )(
        row_data,
        row_baseline.reshape(16, 128),
        pair_table.T,
        lengths.reshape(32, 128),
        model_vis.reshape(AR * AC, 128),
        gains,
        jnp.array([[32 * z + 16 * core + 4 * x + y for z, core, x, y in ORDER]], F32),
    )


def solution(mesh):
    rows = P(("arow", "acol"))
    placed = (
        P(("arow", "acol"), None),
        rows,
        P(("arow", "acol"), None),
        rows,
        P("arow", "acol", None),
        P(("arow", "acol"), None),
    )
    return jax.shard_map(
        local_step, mesh=mesh, in_specs=placed, out_specs=P(("arow", "acol"), None), check_vma=False
    )
```
